256 devices in a mesh: groups: 2 (over y), ctx: 16 (over z), head: 4 (over x), pair: 2 (over core).
Axes of the slice: x: 4, y: 2, z: 16, core: 2. Of those that a mesh axis runs over, the one named last changes fastest.
The devices are a block of a 4x16x16 slice.
Arguments:
- queries: bfloat16 [512, 32, 128], P('groups', 'head'), parts along dimension 0, may hold values from -80 to 80
- prompt_keys: bfloat16 [131072, 4, 128], P(('groups', 'ctx', 'pair'), 'head'), parts along dimension 0, may hold values from -32 to 32
- prompt_values: bfloat16 [131072, 4, 128], P(('groups', 'ctx', 'pair'), 'head'), parts along dimension 0, may hold values from -6 to 6
- residual: bfloat16 [512, 2048], P(('groups', 'ctx', 'head', 'pair')), parts along dimension 0, may hold values from -0.59765625 to 0.59765625
- out_weight: bfloat16 [4096, 2048], P('head', 'ctx'), may hold values from -0.09375 to 0.09375
- norm_gain: float32 [2048], replicated, may hold values from 0.1 to 1.9
- expert_lists: int32 [512, 8], P(('groups', 'ctx')), parts along dimension 0, may hold values from 0 to 127, all different within a row; in each aligned block of 16 rows (0 to 15, 16 to 31, ...) at most 2 rows name the same one
- gate_weights: float32 [512, 8], P(('groups', 'ctx')), parts along dimension 0, may hold values from 0.05 to 0.4
- gate_up: bfloat16 [128, 2048, 1536], P(('ctx', 'head', 'pair')), may hold values from -0.125 to 0.125
- down_proj: bfloat16 [128, 768, 2048], P(('ctx', 'head', 'pair')), may hold values from -0.21875 to 0.21875
Outputs:
- layer_out: bfloat16 [512, 2048], P(('groups', 'ctx', 'head', 'pair')), parts along dimension 0
The draws below stay inside these ranges and needn't reach their ends.
There are 2 independent parts, one for each index of `groups`. The reference program is written for one: setup_inputs(seed, part) draws one part's arguments, and reference() takes and returns one part's arrays. A program takes and returns all parts, laid end to end along the dimension named above; an argument that names none is the same for every part. Nothing has to cross between parts.
Inputs may be any that keep to these rules, and one draw needn't show every extreme that they name: `expert_lists`: A row names 8 different experts. In each aligned block of 16 rows (the rows of one index of ctx) no expert is named by more than 2 rows.
All inputs are finite; a program needn't handle non-finite values.
Results may differ from the reference program's by a relative error of at most 0.018.
Values may be sent and summed in bfloat16 or wider, within the bound.
No kernel may reach another device: no remote copies, remote signals or barrier semaphores. Data moves between devices by JAX's collectives and lax.ppermute only.
A program may use at most 128 MiB of HBM per device.

```python
import math
import jax
import jax.numpy as jnp
import numpy as np
from jax import lax

D = 2048
HEADS = 32
KVH = 4
HD = 128
FFE = 768
TOP = 8
EXPERTS = 128
ROWS = 256
LEN = 65536
ROWS_BLK = 16
CAP = 2


def shared_attention(key):
    position = jnp.arange(LEN, dtype=jnp.float32) / LEN
    base = jnp.clip(jax.random.normal(jax.random.fold_in(key, 101), (LEN, KVH, HD), jnp.float32), -6.0, 6.0)
    queries = jnp.clip(jax.random.normal(jax.random.fold_in(key, 102), (ROWS, HEADS, HD), jnp.float32), -6.0, 6.0)
    keys_out = base * (2.1 + 0.6 * position)[:, None, None]
    return (queries, keys_out)


def draw_queries(key, part):
    return shared_attention(key)[0].astype(jnp.bfloat16)


def draw_prompt_keys(key, part):
    return shared_attention(key)[1].astype(jnp.bfloat16)


def block_scale(stream_key, dims, shards, smallest, largest):
    def one(dim, parts):
        draws = jax.random.uniform(jax.random.fold_in(jax.random.fold_in(stream_key, 6), dim), (parts,), jnp.float32, smallest / len(shards), largest / len(shards))
        return jnp.repeat(jnp.exp(draws), dims[dim] // parts).reshape((-1,) + (1,) * (len(dims) - dim - 1))

    loudness = one(*shards[0])
    for cut in shards[1:]:
        loudness = loudness * one(*cut)
    return loudness


def routed_block(stream_key, own, number, rows, count, top, bound, skew):
    ranking = jax.random.permutation(stream_key, count)
    crowded, usual = load_shares(count, rows * top, bound, skew, True), load_shares(count, rows * top, bound, skew, False)
    places = jnp.arange(count)

    def named(lengths, rotation):
        used = int((lengths > 0).sum())
        fixed = max(1, used // 4)
        passed = fixed + (places - fixed + rotation * (used - fixed)) % max(1, count - fixed)
        return jnp.zeros((count,), jnp.int32).at[ranking[jnp.where(places < fixed, places, passed)]].set(jnp.asarray(lengths, jnp.int32))

    lengths = jnp.where(number % 4 == 0, named(crowded, number // 4), named(usual, number - number // 4 - 1))
    mixed = jax.random.permutation(jax.random.fold_in(own, 3), count)
    source_of, receiver = mixed[0:count // 2 * 2:2], mixed[1:count // 2 * 2:2]
    room = jnp.minimum(lengths[source_of] - 1, bound - lengths[receiver]) // 2
    room = jnp.where((source_of == ranking[0]) | (receiver == ranking[0]) | (lengths[receiver] == 0), 0, jnp.maximum(room, 0))
    passed = jax.random.randint(jax.random.fold_in(own, 4), (count // 2,), 0, 1 << 20) % (room + 1)
    lengths = lengths.at[source_of].add(-passed).at[receiver].add(passed)
    members = jnp.searchsorted(jnp.cumsum(lengths), jnp.arange(rows * top), side="right").astype(jnp.int32)
    table = members.reshape(top, rows).T
    table = table[jax.random.permutation(jax.random.fold_in(own, 1), rows)]
    rotation = jax.random.randint(jax.random.fold_in(own, 2), (rows, 1), 0, top)
    return jnp.take_along_axis(table, (jnp.arange(top)[None, :] + rotation) % top, axis=1)


def load_shares(amount, total, most, skew, full):
    loads = [(1 << 20) // math.isqrt(rank ** skew) + 1 for rank in range(1, amount + 1)]
    largest = most if full else min(most, max(-(-total // amount), total * loads[0] // sum(loads)))
    least = 1 if total - largest >= amount - 1 else 0
    counts, rest = [largest] + [least] * (amount - 1), total - largest - least * (amount - 1)
    while rest > 0:
        free = [i for i in range(1, amount) if counts[i] < largest] or [i for i in range(1, amount) if counts[i] < most]
        mass, left = sum([loads[i] for i in free]), rest
        for i in free:
            addition = min(most - counts[i], max(1, left * loads[i] // mass), rest)
            counts[i] = counts[i] + addition
            rest = rest - addition
    return np.array(counts)


def gaussian(key, extent, scale, bound, cuts=(), held_as=jnp.bfloat16):
    values = jax.random.normal(key, extent, jnp.float32) * scale
    if len(cuts) > 0:
        values = block_scale(key, extent, cuts, -0.22, 0.18) * values
    return jnp.clip(values, min=-bound, max=bound).astype(held_as)


def setup_inputs(seed: int = 0, part: int = 0) -> dict:
    key_list = jax.random.split(jax.random.key(seed), 11)
    part_keys = jax.random.split(jax.random.fold_in(key_list[10], part), 11)
    queries = draw_queries(jax.random.fold_in(jax.random.fold_in(key_list[10], part), 71), part)
    prompt_keys = draw_prompt_keys(jax.random.fold_in(jax.random.fold_in(key_list[10], part), 71), part)
    prompt_values = gaussian(part_keys[2], (LEN, KVH, HD), 1.0, 6.0, ((0, 32), (1, 4)))
    residual = gaussian(part_keys[3], (ROWS, D), 0.1, 0.59765625, ((0, 128),))
    out_weight = gaussian(key_list[4], (HEADS * HD, D), (HEADS * HD) ** -0.5, 0.09375, ((0, 4), (1, 16)))
    norm_gain = jnp.clip(1.0 + 0.18 * jax.random.normal(key_list[5], (D,), jnp.float32), 0.1, 1.9)
    expert_lists_keys = jax.random.split(jax.random.fold_in(part_keys[6], 1), ROWS // ROWS_BLK)
    expert_lists_turns = jax.random.permutation(jax.random.fold_in(part_keys[6], 3), ROWS // ROWS_BLK)
    expert_lists = jax.vmap(lambda own, number: routed_block(jax.random.fold_in(part_keys[6], 2), own, number, ROWS_BLK, EXPERTS, TOP, CAP, 2))(expert_lists_keys, expert_lists_turns).reshape((ROWS, TOP))
    gate_weights = jnp.clip(0.05 + 0.35 * jax.random.uniform(part_keys[7], (ROWS, TOP), jnp.float32) ** block_scale(part_keys[7], (ROWS, TOP), ((0, 16),), -0.2, 0.2), 0.05, 0.4)
    gate_up = gaussian(key_list[8], (EXPERTS, D, 2 * FFE), D ** -0.5, 0.125, ((0, 128),))
    down_proj = gaussian(key_list[9], (EXPERTS, FFE, D), FFE ** -0.5, 0.21875, ((0, 128),))
    return dict(queries=queries, prompt_keys=prompt_keys, prompt_values=prompt_values, residual=residual, out_weight=out_weight, norm_gain=norm_gain, expert_lists=expert_lists, gate_weights=gate_weights, gate_up=gate_up, down_proj=down_proj)


def attend(queries, prompt_keys, prompt_values):
    rows_all = queries.shape[0]
    group = HEADS // KVH
    block = min(1024, LEN)
    scale_factor = 1.0 / math.sqrt(HD)

    def per_head(index):
        query_rows = lax.dynamic_slice_in_dim(queries, index * group, group, 1).reshape(rows_all * group, HD)
        key_head = lax.dynamic_index_in_dim(prompt_keys, index, 1, keepdims=False)
        value_head = lax.dynamic_index_in_dim(prompt_values, index, 1, keepdims=False)
        key_blocks = key_head.reshape(LEN // block, block, HD)
        value_blocks = value_head.reshape(LEN // block, block, HD)

        def step(carry, pieces):
            running, total, numer = carry
            key_piece, value_piece = pieces
            scores = jnp.dot(query_rows, key_piece.T, preferred_element_type=jnp.float32) * scale_factor
            fresh = jnp.maximum(running, lax.optimization_barrier(jnp.max(scores, axis=1)))
            decay = jnp.exp(running - fresh)
            weights = jnp.exp(scores - fresh[:, None])
            total = total * decay + lax.optimization_barrier(jnp.sum(weights, axis=1))
            numer = numer * decay[:, None] + jnp.dot(weights.astype(jnp.bfloat16), value_piece, preferred_element_type=jnp.float32)
            return ((fresh, total, numer), None)
        count = rows_all * group
        start = (jnp.full((count,), -jnp.inf, jnp.float32), jnp.zeros((count,), jnp.float32), jnp.zeros((count, HD), jnp.float32))
        (running, total, numer), unused = lax.scan(step, start, (key_blocks, value_blocks))
        return (numer / total[:, None]).reshape(rows_all, group, HD)
    outputs = lax.map(per_head, jnp.arange(KVH, dtype=jnp.int32))
    return jnp.transpose(outputs, (1, 0, 2, 3)).reshape(rows_all, HEADS * HD)

def expert_apply(inputs, weight_both, weight_down):
    both = jnp.dot(inputs, weight_both, preferred_element_type=jnp.float32)
    inner = (jax.nn.silu(both[:, :FFE]) * both[:, FFE:]).astype(jnp.bfloat16)
    return jnp.dot(inner, weight_down, preferred_element_type=jnp.float32).astype(jnp.bfloat16)

def reference(queries, prompt_keys, prompt_values, residual, out_weight, norm_gain, expert_lists, gate_weights, gate_up, down_proj):
    attended = attend(queries, prompt_keys, prompt_values).astype(jnp.bfloat16)
    projected = jnp.dot(attended, out_weight, preferred_element_type=jnp.float32)
    hidden_state = (residual.astype(jnp.float32) + projected).astype(jnp.bfloat16)
    as_float = hidden_state.astype(jnp.float32)
    normed = (as_float * lax.rsqrt(lax.optimization_barrier(jnp.mean(as_float * as_float, axis=1, keepdims=True)) + 1e-06) * norm_gain).astype(jnp.bfloat16)
    slots_most = ROWS // ROWS_BLK * CAP

    def per_expert(carry, index):
        hits = expert_lists == index
        weight_row = lax.optimization_barrier(jnp.sum(jnp.where(hits, gate_weights, jnp.zeros_like(gate_weights)), axis=1))
        chosen = jnp.any(hits, axis=1)
        picked = jnp.nonzero(chosen, size=slots_most, fill_value=0)[0].astype(jnp.int32)
        valid = jnp.arange(slots_most, dtype=jnp.int32) < jnp.sum(chosen.astype(jnp.int32))
        weight_both = lax.dynamic_index_in_dim(gate_up, index, 0, keepdims=False)
        weight_down = lax.dynamic_index_in_dim(down_proj, index, 0, keepdims=False)
        produced = expert_apply(normed[picked], weight_both, weight_down)
        factor = jnp.where(valid, weight_row[picked], jnp.zeros_like(weight_row[picked]))
        contrib = produced.astype(jnp.float32) * factor[:, None]
        return (carry.at[picked].add(contrib), None)
    mixture, unused = lax.scan(per_expert, jnp.zeros((ROWS, D), jnp.float32), jnp.arange(EXPERTS, dtype=jnp.int32))
    return (hidden_state.astype(jnp.float32) + mixture).astype(jnp.bfloat16)
```

```python
import math

import jax
import jax.numpy as jnp
from jax import lax
from jax.experimental import pallas as pl
from jax.experimental.pallas import tpu as pltpu
from jax.sharding import PartitionSpec as P

F32 = jnp.float32
BF16 = jnp.bfloat16
STATS = 8


def iota(shape, dim):
    return lax.broadcasted_iota(jnp.int32, shape, dim)


def dot(a, b):
    return lax.dot_general(a, b, (((1,), (0,)), ((), ())), preferred_element_type=F32)


def as_row(column, lanes):
    n = column.shape[0]
    here = iota((n, lanes), 0) == iota((n, lanes), 1)
    return jnp.sum(jnp.where(here, jnp.broadcast_to(column, (n, lanes)), 0.0), axis=0, keepdims=True)


def as_column(row, n):
    lanes = row.shape[1]
    here = iota((n, lanes), 0) == iota((n, lanes), 1)
    return jnp.sum(jnp.where(here, jnp.broadcast_to(row, (n, lanes)), 0.0), axis=1, keepdims=True)


def pieces(row):
    first = row.astype(BF16).astype(F32)
    second = (row - first).astype(BF16).astype(F32)
    third = row - first - second
    return first, second, third


def stacked(rows, lanes):
    at = iota((STATS, lanes), 0)
    out = jnp.zeros((STATS, lanes), F32)
    for i, row in enumerate(rows):
        out = jnp.where(at == i, jnp.broadcast_to(row, (STATS, lanes)), out)
    return out


def attend_half(half, queries, keys, values, blocks, pairs_block):
    units, _, unit, width = queries.shape
    length = keys.shape[0]
    tile_blocks = max(1, 256 // pairs_block)
    steps = blocks // tile_blocks
    tile_units = units // steps
    tile = tile_units * unit
    scale = 1.0 / math.sqrt(width)

    def kernel(half_ref, q_ref, k_ref, v_ref, o_ref):
        q = q_ref[:, 0].reshape(tile, width)
        scores = lax.dot_general(q, k_ref[...], (((1,), (1,)), ((), ())), preferred_element_type=F32)
        top = jnp.max(scores, axis=1, keepdims=True)
        probs = jnp.exp((scores - top) * scale)
        total = jnp.sum(probs, axis=1, keepdims=True)
        out = dot(probs.astype(BF16), v_ref[...]) / total
        level = top * scale + jnp.log(total)
        for b in range(tile_blocks):
            part = slice(b * pairs_block, (b + 1) * pairs_block)
            o_ref[b, 0:pairs_block, :] = out[part].astype(BF16)
            row = as_row(level[part], width)
            o_ref[b, pairs_block : pairs_block + STATS, :] = stacked(pieces(row), width).astype(BF16)

    return pl.pallas_call(
        kernel,
        grid_spec=pltpu.PrefetchScalarGridSpec(
            num_scalar_prefetch=1,
            grid=(steps,),
            in_specs=[
                pl.BlockSpec((tile_units, 1, unit, width), lambda i, half: (i, half[0], 0, 0)),
                pl.BlockSpec((length, width), lambda i, half: (0, 0)),
                pl.BlockSpec((length, width), lambda i, half: (0, 0)),
            ],
            out_specs=pl.BlockSpec((tile_blocks, pairs_block + STATS, width), lambda i, half: (i, 0, 0)),
        ),
        out_shape=jax.ShapeDtypeStruct((blocks, pairs_block + STATS, width), BF16),
        compiler_params=pltpu.CompilerParams(vmem_limit_bytes=48 << 20),
        name="attend",
    )(half, queries, keys, values)


def levels_of(ref, pairs_block):
    stats = ref[:, pairs_block : pairs_block + STATS, :].astype(F32)
    return stats[:, 0, :] + stats[:, 1, :] + stats[:, 2, :]


def merge_pair(mine, other, residual, names):
    blocks, height, width = mine.shape
    pairs_block = height - STATS

    def kernel(a_ref, b_ref, r_ref, n_ref, o_ref):
        level_a, level_b = levels_of(a_ref, pairs_block), levels_of(b_ref, pairs_block)
        top = jnp.maximum(level_a, level_b)
        share_a, share_b = jnp.exp(level_a - top), jnp.exp(level_b - top)
        total = share_a + share_b
        share_a, share_b = share_a / total, share_b / total
        level = top + jnp.log(total)
        first, second, third = pieces(level)
        residual_all = r_ref[...].astype(F32)
        listed = n_ref[...]
        for b in range(blocks):
            col_a, col_b = as_column(share_a[b : b + 1], pairs_block), as_column(share_b[b : b + 1], pairs_block)
            both = a_ref[b, 0:pairs_block, :].astype(F32) * col_a + b_ref[b, 0:pairs_block, :].astype(F32) * col_b
            o_ref[b, 0:pairs_block, :] = both.astype(BF16)
            own = residual_all[:, b * width : (b + 1) * width]
            rows = (first[b : b + 1], second[b : b + 1], third[b : b + 1], own[0:1], own[1:2], listed)
            o_ref[b, pairs_block:height, :] = stacked(rows, width).astype(BF16)

    return pl.pallas_call(
        kernel, out_shape=jax.ShapeDtypeStruct((blocks, height, width), BF16), name="merge_pair"
    )(mine, other, residual, names)


def combine_all(parts, rows_half, heads):
    sources, height, width = parts.shape
    pairs_block = height - STATS

    def kernel(x_ref, o_ref, acc_ref):
        level = levels_of(x_ref, pairs_block)
        share = jnp.exp(level - jnp.max(level, axis=0, keepdims=True))
        share = share / jnp.sum(share, axis=0, keepdims=True)
        acc = jnp.zeros((pairs_block, width), F32)
        for s in range(sources):
            acc = acc + x_ref[s, 0:pairs_block, :].astype(F32) * as_column(share[s : s + 1], pairs_block)
        acc_ref[...] = acc
        by_head = [acc_ref[pl.ds(h, rows_half, stride=heads), :] for h in range(heads)]
        attended = jnp.concatenate(by_head, axis=0).astype(BF16)
        for s in range(sources):
            o_ref[s] = attended

    return pl.pallas_call(
        kernel,
        out_shape=jax.ShapeDtypeStruct((sources, pairs_block, width), BF16),
        scratch_shapes=[pltpu.VMEM((pairs_block, width), F32)],
        name="combine_all",
    )(parts)


def project(attended, weight, parts, place, rows_half, heads, copies):
    blocks, pairs_block, width = attended.shape
    columns = weight.shape[1]
    rows = blocks * rows_half

    def kernel(place_ref, a_ref, w_ref, s_ref, o_ref):
        a = a_ref[...].astype(F32)
        by_head = [a[:, h * rows_half : (h + 1) * rows_half, :].reshape(rows, width) for h in range(heads)]
        out = dot(jnp.concatenate(by_head, axis=1).astype(BF16), w_ref[...])
        out = out.reshape(blocks, rows_half, columns)
        stats = s_ref[...].astype(F32)
        at = iota((blocks, rows_half, columns), 1)
        first = 2 * place_ref[0]
        out = out + jnp.where(at == first, stats[:, 3:4, :], 0.0) + jnp.where(at == first + 1, stats[:, 4:5, :], 0.0)
        out = out.reshape(rows, columns).astype(BF16)
        for i in range(copies):
            o_ref[i] = out

    height = parts.shape[1]
    return pl.pallas_call(
        kernel,
        grid_spec=pltpu.PrefetchScalarGridSpec(
            num_scalar_prefetch=1,
            grid=(1,),
            in_specs=[
                pl.BlockSpec(attended.shape, lambda i, place: (0, 0, 0)),
                pl.BlockSpec(weight.shape, lambda i, place: (0, 0)),
                pl.BlockSpec((blocks, STATS, width), lambda i, place: (0, (height - STATS) // STATS, 0)),
            ],
            out_specs=pl.BlockSpec((copies, rows, columns), lambda i, place: (0, 0, 0)),
        ),
        out_shape=jax.ShapeDtypeStruct((copies, rows, columns), BF16),
        name="project",
    )(place, attended, weight, parts)


def selection(parts, place, sizes):
    n_ctx, n_head, n_pair, rows_own, top, capacity = sizes
    block_rows = n_head * n_pair * rows_own
    rows_all = n_ctx * block_rows
    blocks, height, width = parts.shape
    per_peer = n_ctx * capacity
    owned = 8

    def natural(lane):
        pair = lane // (rows_all // n_pair)
        rest = lane % (rows_all // n_pair)
        block = rest // (n_head * rows_own)
        head = (rest // rows_own) % n_head
        return block, (head * n_pair + pair) * rows_own + rest % rows_own

    def kernel(place_ref, s_ref, d_ref, o_ref):
        listed = s_ref[...].astype(F32)[:, 5, :]
        count = n_ctx * n_ctx
        repeated = jnp.concatenate([listed] * n_ctx, axis=0)
        expert = (iota((count, width), 0) // n_ctx * n_head * n_pair + place_ref[0] * n_pair + place_ref[1]).astype(F32)
        equal = (repeated == expert).astype(F32).astype(BF16)
        fold = (iota((width, block_rows), 0) // top == iota((width, block_rows), 1)).astype(F32).astype(BF16)
        hits = dot(equal, fold)
        earlier = (iota((block_rows, block_rows), 0) < iota((block_rows, block_rows), 1)).astype(F32).astype(BF16)
        rank = dot(hits.astype(BF16), earlier)
        slot = jnp.where(hits > 0.5, rank + 1.0, 0.0).astype(BF16)
        expand = iota((count * capacity, count), 0) // capacity == iota((count * capacity, count), 1)
        slot = dot(expand.astype(F32).astype(BF16), slot).astype(BF16)
        block, row = natural(iota((block_rows, rows_all), 1))
        spread = (iota((block_rows, rows_all), 0) == row).astype(F32).astype(BF16)
        slot = dot(slot, spread)
        at = iota((count * capacity, rows_all), 0)
        block, row = natural(iota((count * capacity, rows_all), 1))
        mine = (block == (at // capacity) % n_ctx) & (slot == (at % capacity + 1).astype(F32))
        d_ref[...] = mine.astype(F32).astype(BF16)
        at = iota((n_ctx * owned, rows_all), 0)
        block, row = natural(iota((n_ctx * owned, rows_all), 1))
        first = (place_ref[0] * n_pair + place_ref[1]) * rows_own
        mine = (block == at // owned) & (row == first + at % owned) & (at % owned < rows_own)
        o_ref[...] = mine.astype(F32).astype(BF16)

    return pl.pallas_call(
        kernel,
        grid_spec=pltpu.PrefetchScalarGridSpec(
            num_scalar_prefetch=1,
            grid=(1,),
            in_specs=[pl.BlockSpec((blocks, STATS, width), lambda i, place: (0, (height - STATS) // STATS, 0))],
            out_specs=[
                pl.BlockSpec((n_ctx * per_peer, rows_all), lambda i, place: (0, 0)),
                pl.BlockSpec((n_ctx * owned, rows_all), lambda i, place: (0, 0)),
            ],
        ),
        out_shape=[
            jax.ShapeDtypeStruct((n_ctx * per_peer, rows_all), BF16),
            jax.ShapeDtypeStruct((n_ctx * owned, rows_all), BF16),
        ],
        name="selection",
    )(place, parts)


def dispatch(partials, picks, owns, n_ctx, n_head, n_pair):
    copies, rows, columns = partials.shape
    per_peer, owned = picks.shape[0] // n_ctx, owns.shape[0] // n_ctx

    def kernel(x_ref, d_ref, w_ref, o_ref):
        halves = []
        for p in range(n_pair):
            acc = x_ref[p].astype(F32)
            for h in range(1, n_head):
                acc = acc + x_ref[h * n_pair + p].astype(F32)
            halves.append(acc)
        hidden = jnp.concatenate(halves, axis=0).astype(BF16)
        sent = dot(d_ref[...], hidden).reshape(n_ctx, per_peer, columns)
        kept = dot(w_ref[...], hidden).reshape(n_ctx, owned, columns)
        o_ref[:, 0:per_peer, :] = sent.astype(BF16)
        o_ref[:, per_peer : per_peer + owned, :] = kept.astype(BF16)

    return pl.pallas_call(
        kernel, out_shape=jax.ShapeDtypeStruct((n_ctx, per_peer + owned, columns), BF16), name="dispatch"
    )(partials, picks, owns)


def norm_rows(parts, gain, per_peer):
    sources, height, columns = parts.shape
    owned = height - per_peer
    width = sources * columns

    def kernel(x_ref, g_ref, n_ref, o_ref):
        whole = jnp.concatenate([x_ref[s].astype(F32) for s in range(sources)], axis=1)
        o_ref[...] = whole[per_peer:height]
        rows = whole[0:per_peer]
        mean = jnp.sum(rows * rows, axis=1, keepdims=True) * (1.0 / width)
        n_ref[...] = (rows * lax.rsqrt(mean + 1e-06) * g_ref[...]).astype(BF16)

    return pl.pallas_call(
        kernel,
        out_shape=[jax.ShapeDtypeStruct((per_peer, width), BF16), jax.ShapeDtypeStruct((owned, width), F32)],
        name="norm_rows",
    )(parts, gain.reshape(1, width))


def weigh(returned, lists, weights, place, sizes):
    n_ctx, n_head, n_pair, rows_own, top, capacity = sizes
    slots, width = returned.shape
    rows = lists.shape[0]

    def kernel(place_ref, x_ref, l_ref, g_ref, o_ref):
        lane = iota((rows, slots), 1)
        expert = lane // capacity * n_head * n_pair + place_ref[0] * n_pair + place_ref[1]
        hits = jnp.zeros((rows, slots), F32)
        factor = jnp.zeros((rows, slots), F32)
        for k in range(top):
            same = l_ref[:, k : k + 1] == expert
            hits = jnp.where(same, 1.0, hits)
            factor = jnp.where(same, g_ref[:, k : k + 1], factor)
        earlier = (iota((rows, rows), 1) < iota((rows, rows), 0)).astype(F32).astype(BF16)
        rank = dot(earlier, hits.astype(BF16))
        factor = jnp.where(rank == (lane % capacity).astype(F32), factor, 0.0)
        first, second, third = pieces(factor)
        x = x_ref[...]
        o_ref[...] = dot(first.astype(BF16), x) + dot(second.astype(BF16), x) + dot(third.astype(BF16), x)

    return pl.pallas_call(
        kernel,
        grid_spec=pltpu.PrefetchScalarGridSpec(
            num_scalar_prefetch=1,
            grid=(1,),
            in_specs=[
                pl.BlockSpec((slots, width), lambda i, place: (0, 0)),
                pl.BlockSpec((rows, top), lambda i, place: (0, 0)),
                pl.BlockSpec((rows, top), lambda i, place: (0, 0)),
            ],
            out_specs=pl.BlockSpec((rows, width), lambda i, place: (0, 0)),
        ),
        out_shape=jax.ShapeDtypeStruct((rows, width), F32),
        name="weigh",
    )(place, returned, lists, weights)


def body(
    queries,
    prompt_keys,
    prompt_values,
    residual,
    out_weight,
    norm_gain,
    expert_lists,
    gate_weights,
    gate_up,
    down_proj,
):
    n_ctx = lax.axis_size("ctx")
    n_head = lax.axis_size("head")
    n_pair = lax.axis_size("pair")
    rows_own, width = residual.shape
    rows_all, heads, head_size = queries.shape
    block_rows, top = expert_lists.shape
    capacity = 2
    rows_half = n_head * rows_own
    pairs_block = rows_half * heads
    sizes = (n_ctx, n_head, n_pair, rows_own, top, capacity)
    head, pair = lax.axis_index("head"), lax.axis_index("pair")
    place = jnp.stack([head, pair]).astype(jnp.int32)

    units = queries.reshape(n_ctx * n_head, n_pair, rows_own * heads, head_size)
    keys = prompt_keys.reshape(-1, head_size)
    values = prompt_values.reshape(-1, head_size)
    theirs = attend_half((1 - pair).reshape(1), units, keys, values, n_ctx, pairs_block)
    swapped = lax.ppermute(theirs, "pair", [(0, 1), (1, 0)])
    ours = attend_half(pair.reshape(1), units, keys, values, n_ctx, pairs_block)
    names = expert_lists.astype(F32).reshape(1, block_rows * top)
    merged = merge_pair(ours, swapped, residual, names)
    parts = lax.all_to_all(merged, "ctx", 0, 0, tiled=True)
    copies = combine_all(parts, rows_half, heads)
    picks, owns = selection(parts, place, sizes)
    attended = lax.all_to_all(copies, "ctx", 0, 0, tiled=True)
    partial = project(attended, out_weight, parts, place, rows_half, heads, n_head * n_pair)
    partials = lax.all_to_all(partial, ("head", "pair"), 0, 0, tiled=True)
    sending = dispatch(partials, picks, owns, n_ctx, n_head, n_pair)
    arrived = lax.all_to_all(sending, "ctx", 0, 0, tiled=True)
    normed, own = norm_rows(arrived, norm_gain, n_ctx * capacity)
    hidden_units = down_proj.shape[1]
    both = jnp.dot(normed, gate_up[0], preferred_element_type=F32)
    inner = (jax.nn.silu(both[:, :hidden_units]) * both[:, hidden_units:]).astype(BF16)
    produced = jnp.dot(inner, down_proj[0], preferred_element_type=F32).astype(BF16)
    returned = lax.all_to_all(produced.reshape(n_ctx, capacity, width), "ctx", 0, 0, tiled=True)
    weighted = weigh(returned.reshape(n_ctx * capacity, width), expert_lists, gate_weights, place, sizes)
    shares = lax.all_to_all(weighted.reshape(n_head * n_pair, rows_own, width), ("head", "pair"), 0, 0, tiled=True)
    return (own[:rows_own] + jnp.sum(shares, axis=0)).astype(BF16)


def solution(mesh):
    in_specs = (
        P("groups", "head", None),
        P(("groups", "ctx", "pair"), "head", None),
        P(("groups", "ctx", "pair"), "head", None),
        P(("groups", "ctx", "head", "pair"), None),
        P("head", "ctx"),
        P(),
        P(("groups", "ctx"), None),
        P(("groups", "ctx"), None),
        P(("ctx", "head", "pair"), None, None),
        P(("ctx", "head", "pair"), None, None),
    )
    out_specs = P(("groups", "ctx", "head", "pair"), None)
    return jax.shard_map(body, mesh=mesh, in_specs=in_specs, out_specs=out_specs, check_vma=False)
```

```python
import math

import jax
import jax.numpy as jnp
from jax import lax
from jax.experimental import pallas as pl
from jax.experimental.pallas import tpu as pltpu
from jax.sharding import PartitionSpec as P

F32 = jnp.float32
BF16 = jnp.bfloat16
LIMIT = 16 << 20
STATS = 8


SMEM = pl.BlockSpec(memory_space=pltpu.SMEM)
VMEM = pl.BlockSpec(memory_space=pltpu.VMEM)
HBM = pl.BlockSpec(memory_space=pltpu.HBM)


def in_hbm(x):
    return pltpu.with_memory_space_constraint(x, pltpu.HBM)


def iota(shape, dim):
    return lax.broadcasted_iota(jnp.int32, shape, dim)


def dot(a, b):
    return lax.dot_general(a, b, (((1,), (0,)), ((), ())), preferred_element_type=F32)


def as_row(column, lanes):
    n = column.shape[0]
    here = iota((n, lanes), 0) == iota((n, lanes), 1)
    return jnp.sum(jnp.where(here, jnp.broadcast_to(column, (n, lanes)), 0.0), axis=0, keepdims=True)


def as_column(row, n):
    lanes = row.shape[1]
    here = iota((n, lanes), 0) == iota((n, lanes), 1)
    return jnp.sum(jnp.where(here, jnp.broadcast_to(row, (n, lanes)), 0.0), axis=1, keepdims=True)


def pieces(row):
    first = row.astype(BF16).astype(F32)
    second = (row - first).astype(BF16).astype(F32)
    third = row - first - second
    return first, second, third


def stacked(rows, lanes):
    at = iota((STATS, lanes), 0)
    out = jnp.zeros((STATS, lanes), F32)
    for i, row in enumerate(rows):
        out = jnp.where(at == i, jnp.broadcast_to(row, (STATS, lanes)), out)
    return out


def attend_half(half, queries, keys, values, blocks, pairs_block):
    units, _, unit, width = queries.shape
    length = keys.shape[0]
    tile_blocks = max(1, 256 // pairs_block)
    steps = blocks // tile_blocks
    tile_units = units // steps
    tile = tile_units * unit
    scale = 1.0 / math.sqrt(width)

    def kernel(half_ref, q_hbm, k_hbm, v_hbm, o_ref, q_ref, k_ref, v_ref, sems):
        copy_k = pltpu.make_async_copy(k_hbm, k_ref, sems.at[0])
        copy_q = pltpu.make_async_copy(q_hbm.at[:, half_ref[0]], q_ref, sems.at[1])
        copy_v = pltpu.make_async_copy(v_hbm, v_ref, sems.at[2])
        copy_q.start()
        copy_k.start()
        copy_v.start()
        copy_q.wait()
        copy_k.wait()
        copy_v.wait()

        def step(i, carry):
            q = q_ref[pl.ds(i * tile_units, tile_units)].reshape(tile, width)
            scores = lax.dot_general(q, k_ref[...], (((1,), (1,)), ((), ())), preferred_element_type=F32)
            top = jnp.max(scores, axis=1, keepdims=True)
            probs = jnp.exp((scores - top) * scale)
            total = jnp.sum(probs, axis=1, keepdims=True)
            out = dot(probs.astype(BF16), v_ref[...]) / total
            level = top * scale + jnp.log(total)
            for b in range(tile_blocks):
                part = slice(b * pairs_block, (b + 1) * pairs_block)
                at = i * tile_blocks + b
                o_ref[at, 0:pairs_block, :] = out[part].astype(BF16)
                row = as_row(level[part], width)
                o_ref[at, pairs_block : pairs_block + STATS, :] = stacked(pieces(row), width).astype(BF16)
            return carry

        lax.fori_loop(0, steps, step, 0)

    return pl.pallas_call(
        kernel,
        in_specs=[SMEM, HBM, HBM, HBM],
        out_specs=VMEM,
        out_shape=jax.ShapeDtypeStruct((blocks, pairs_block + STATS, width), BF16),
        scratch_shapes=[
            pltpu.VMEM((units, unit, width), BF16),
            pltpu.VMEM((length, width), BF16),
            pltpu.VMEM((length, width), BF16),
            pltpu.SemaphoreType.DMA((3,)),
        ],
        compiler_params=pltpu.CompilerParams(vmem_limit_bytes=24 << 20),
        name="attend",
    )(half, in_hbm(queries), in_hbm(keys), in_hbm(values))


def levels_of(ref, pairs_block):
    stats = ref[:, pairs_block : pairs_block + STATS, :].astype(F32)
    return stats[:, 0, :] + stats[:, 1, :] + stats[:, 2, :]


def merge_pair(mine, other, residual, names):
    blocks, height, width = mine.shape
    pairs_block = height - STATS

    def kernel(a_ref, b_ref, r_hbm, n_hbm, o_ref, r_ref, n_ref, sems):
        copy_r = pltpu.make_async_copy(r_hbm, r_ref, sems.at[0])
        copy_n = pltpu.make_async_copy(n_hbm, n_ref, sems.at[1])
        copy_r.start()
        copy_n.start()
        level_a, level_b = levels_of(a_ref, pairs_block), levels_of(b_ref, pairs_block)
        highest = jnp.maximum(level_a, level_b)
        share_a, share_b = jnp.exp(level_a - highest), jnp.exp(level_b - highest)
        total = share_a + share_b
        share_a, share_b = share_a / total, share_b / total
        level = highest + jnp.log(total)
        first, second, third = pieces(level)
        for b in range(blocks):
            col_a, col_b = as_column(share_a[b : b + 1], pairs_block), as_column(share_b[b : b + 1], pairs_block)
            both = a_ref[b, 0:pairs_block, :].astype(F32) * col_a + b_ref[b, 0:pairs_block, :].astype(F32) * col_b
            o_ref[b, 0:pairs_block, :] = both.astype(BF16)
        copy_r.wait()
        copy_n.wait()
        residual_all = r_ref[...].astype(F32)
        top, rows = n_ref.shape
        spread = (iota((rows, width), 1) % rows == iota((rows, width), 0)).astype(F32).astype(BF16)
        listed = dot(n_ref[...].astype(F32).astype(BF16), spread)
        listed = jnp.where(iota((top, width), 1) // rows == iota((top, width), 0), listed, 0.0)
        listed = jnp.sum(listed, axis=0, keepdims=True)
        for b in range(blocks):
            own = residual_all[:, b * width : (b + 1) * width]
            rows_b = (first[b : b + 1], second[b : b + 1], third[b : b + 1], own[0:1], own[1:2], listed)
            o_ref[b, pairs_block:height, :] = stacked(rows_b, width).astype(BF16)

    return pl.pallas_call(
        kernel,
        in_specs=[VMEM, VMEM, HBM, HBM],
        out_shape=jax.ShapeDtypeStruct((blocks, height, width), BF16),
        scratch_shapes=[
            pltpu.VMEM(residual.shape, residual.dtype),
            pltpu.VMEM(names.shape, names.dtype),
            pltpu.SemaphoreType.DMA((2,)),
        ],
        compiler_params=pltpu.CompilerParams(vmem_limit_bytes=LIMIT),
        name="merge_pair",
    )(mine, other, in_hbm(residual), in_hbm(names))


def combine_all(parts, rows_half, heads):
    sources, height, width = parts.shape
    pairs_block = height - STATS

    def kernel(x_ref, o_hbm, acc_ref, att_ref, sem):
        level = levels_of(x_ref, pairs_block)
        share = jnp.exp(level - jnp.max(level, axis=0, keepdims=True))
        share = share / jnp.sum(share, axis=0, keepdims=True)
        acc = jnp.zeros((pairs_block, width), F32)
        for s in range(sources):
            acc = acc + x_ref[s, 0:pairs_block, :].astype(F32) * as_column(share[s : s + 1], pairs_block)
        acc_ref[...] = acc
        by_head = [acc_ref[pl.ds(h, rows_half, stride=heads), :] for h in range(heads)]
        att_ref[...] = jnp.concatenate(by_head, axis=0).astype(BF16)
        copies = [pltpu.make_async_copy(att_ref, o_hbm.at[s], sem.at[s]) for s in range(sources)]
        for copy in copies:
            copy.start()
        for copy in copies:
            copy.wait()

    return pl.pallas_call(
        kernel,
        in_specs=[VMEM],
        out_specs=HBM,
        out_shape=pltpu.HBM((sources, pairs_block, width), BF16),
        scratch_shapes=[
            pltpu.VMEM((pairs_block, width), F32),
            pltpu.VMEM((pairs_block, width), BF16),
            pltpu.SemaphoreType.DMA((sources,)),
        ],
        compiler_params=pltpu.CompilerParams(vmem_limit_bytes=LIMIT),
        name="combine_all",
    )(parts)


def project(attended, weight, parts, place, rows_half, heads, copies):
    blocks, pairs_block, width = attended.shape
    columns = weight.shape[1]
    rows = blocks * rows_half

    def kernel(place_ref, a_ref, w_ref, s_ref, o_ref):
        a = a_ref[...].astype(F32)
        by_head = [a[:, h * rows_half : (h + 1) * rows_half, :].reshape(rows, width) for h in range(heads)]
        out = dot(jnp.concatenate(by_head, axis=1).astype(BF16), w_ref[...])
        out = out.reshape(blocks, rows_half, columns)
        stats = s_ref[:, pairs_block : pairs_block + STATS, :].astype(F32)
        at = iota((blocks, rows_half, columns), 1)
        first = 2 * place_ref[0]
        out = out + jnp.where(at == first, stats[:, 3:4, :], 0.0) + jnp.where(at == first + 1, stats[:, 4:5, :], 0.0)
        out = out.reshape(rows, columns).astype(BF16)
        for i in range(copies):
            o_ref[i] = out

    return pl.pallas_call(
        kernel,
        in_specs=[SMEM, VMEM, VMEM, VMEM],
        out_shape=jax.ShapeDtypeStruct((copies, rows, columns), BF16),
        compiler_params=pltpu.CompilerParams(vmem_limit_bytes=LIMIT),
        name="project",
    )(place, attended, weight, parts)


def selection(parts, place, sizes, fetched):
    n_ctx, n_head, n_pair, rows_own, top, capacity = sizes
    block_rows = n_head * n_pair * rows_own
    rows_all = n_ctx * block_rows
    blocks, height, width = parts.shape
    per_peer = n_ctx * capacity
    owned = 8

    def natural(lane):
        pair = lane // (rows_all // n_pair)
        rest = lane % (rows_all // n_pair)
        block = rest // (n_head * rows_own)
        head = (rest // rows_own) % n_head
        return block, (head * n_pair + pair) * rows_own + rest % rows_own

    count_fetched = len(fetched)

    def kernel(place_ref, s_ref, *refs):
        sources, d_ref, o_ref = refs[:count_fetched], refs[count_fetched], refs[count_fetched + 1]
        targets, sems = refs[count_fetched + 2 : -1], refs[-1]
        fetches = [pltpu.make_async_copy(a, b, sems.at[i]) for i, (a, b) in enumerate(zip(sources, targets))]
        for fetch in fetches:
            fetch.start()
        listed = s_ref[:, height - STATS : height, :].astype(F32)[:, 5, :]
        count = n_ctx * n_ctx
        repeated = jnp.concatenate([listed] * n_ctx, axis=0)
        expert = (iota((count, width), 0) // n_ctx * n_head * n_pair + place_ref[0] * n_pair + place_ref[1]).astype(F32)
        equal = (repeated == expert).astype(F32).astype(BF16)
        fold = (iota((width, block_rows), 0) % block_rows == iota((width, block_rows), 1)).astype(F32).astype(BF16)
        hits = dot(equal, fold)
        earlier = (iota((block_rows, block_rows), 0) < iota((block_rows, block_rows), 1)).astype(F32).astype(BF16)
        rank = dot(hits.astype(BF16), earlier)
        slot = jnp.where(hits > 0.5, rank + 1.0, 0.0).astype(BF16)
        expand = iota((count * capacity, count), 0) // capacity == iota((count * capacity, count), 1)
        slot = dot(expand.astype(F32).astype(BF16), slot).astype(BF16)
        block, row = natural(iota((block_rows, rows_all), 1))
        spread = (iota((block_rows, rows_all), 0) == row).astype(F32).astype(BF16)
        slot = dot(slot, spread)
        at = iota((count * capacity, rows_all), 0)
        block, row = natural(iota((count * capacity, rows_all), 1))
        mine = (block == (at // capacity) % n_ctx) & (slot == (at % capacity + 1).astype(F32))
        d_ref[...] = mine.astype(F32).astype(BF16)
        at = iota((n_ctx * owned, rows_all), 0)
        block, row = natural(iota((n_ctx * owned, rows_all), 1))
        first = (place_ref[0] * n_pair + place_ref[1]) * rows_own
        mine = (block == at // owned) & (row == first + at % owned) & (at % owned < rows_own)
        o_ref[...] = mine.astype(F32).astype(BF16)
        for fetch in fetches:
            fetch.wait()

    return pl.pallas_call(
        kernel,
        in_specs=[SMEM, VMEM] + [HBM] * count_fetched,
        out_specs=[VMEM] * (2 + count_fetched),
        out_shape=[
            jax.ShapeDtypeStruct((n_ctx * per_peer, rows_all), BF16),
            jax.ShapeDtypeStruct((n_ctx * owned, rows_all), BF16),
        ]
        + [jax.ShapeDtypeStruct(x.shape, x.dtype) for x in fetched],
        scratch_shapes=[pltpu.SemaphoreType.DMA((count_fetched,))],
        compiler_params=pltpu.CompilerParams(vmem_limit_bytes=LIMIT),
        name="selection",
    )(place, parts, *[in_hbm(x) for x in fetched])


def dispatch(partials, picks, owns, n_ctx, n_head, n_pair):
    copies, rows, columns = partials.shape
    per_peer, owned = picks.shape[0] // n_ctx, owns.shape[0] // n_ctx

    def kernel(x_ref, d_ref, w_ref, o_ref):
        halves = []
        for p in range(n_pair):
            acc = x_ref[p].astype(F32)
            for h in range(1, n_head):
                acc = acc + x_ref[h * n_pair + p].astype(F32)
            halves.append(acc)
        hidden = jnp.concatenate(halves, axis=0).astype(BF16)
        sent = dot(d_ref[...], hidden).reshape(n_ctx, per_peer, columns)
        kept = dot(w_ref[...], hidden).reshape(n_ctx, owned, columns)
        o_ref[:, 0:per_peer, :] = sent.astype(BF16)
        o_ref[:, per_peer : per_peer + owned, :] = kept.astype(BF16)

    return pl.pallas_call(
        kernel, out_shape=jax.ShapeDtypeStruct((n_ctx, per_peer + owned, columns), BF16), compiler_params=pltpu.CompilerParams(vmem_limit_bytes=LIMIT), name="dispatch"
    )(partials, picks, owns)


def run_expert(parts, gain, gate_up, down, capacity):
    sources, height, columns = parts.shape
    slots = sources * capacity
    owned = height - slots
    width = sources * columns
    units = down.shape[0]
    chunks = 8
    chunk = width // chunks

    def kernel(x_ref, g_ref, up_hbm, down_hbm, y_ref, o_ref, up_ref, down_ref, sems):
        ups = [
            pltpu.make_async_copy(
                up_hbm.at[pl.ds(i * chunk, chunk)], up_ref.at[pl.ds(i * chunk, chunk)], sems.at[i]
            )
            for i in range(chunks)
        ]
        last = pltpu.make_async_copy(down_hbm, down_ref, sems.at[chunks])
        for copy in ups:
            copy.start()
        last.start()
        whole = jnp.concatenate([x_ref[s].astype(F32) for s in range(sources)], axis=1)
        o_ref[...] = whole[slots:height]
        rows = whole[0:slots]
        mean = jnp.sum(rows * rows, axis=1, keepdims=True) * (1.0 / width)
        normed = (rows * lax.rsqrt(mean + 1e-06) * g_ref[...]).astype(BF16)
        both = jnp.zeros((slots, 2 * units), F32)
        for i in range(chunks):
            ups[i].wait()
            both = both + dot(normed[:, i * chunk : (i + 1) * chunk], up_ref[i * chunk : (i + 1) * chunk, :])
        gate = both[:, :units]
        inner = (gate / (1.0 + jnp.exp(-gate)) * both[:, units:]).astype(BF16)
        last.wait()
        y_ref[...] = dot(inner, down_ref[...]).astype(BF16).reshape(sources, capacity, width)

    return pl.pallas_call(
        kernel,
        in_specs=[VMEM, VMEM, HBM, HBM],
        out_shape=[
            jax.ShapeDtypeStruct((sources, capacity, width), BF16),
            jax.ShapeDtypeStruct((owned, width), F32),
        ],
        scratch_shapes=[
            pltpu.VMEM(gate_up.shape, BF16),
            pltpu.VMEM(down.shape, BF16),
            pltpu.SemaphoreType.DMA((chunks + 1,)),
        ],
        compiler_params=pltpu.CompilerParams(vmem_limit_bytes=24 << 20),
        name="run_expert",
    )(parts, gain.reshape(1, width), in_hbm(gate_up), in_hbm(down))


def weigh(returned, lists, weights, place, sizes):
    n_ctx, n_head, n_pair, rows_own, top, capacity = sizes
    slots, width = n_ctx * capacity, returned.shape[2]
    rows = lists.shape[1]

    def kernel(place_ref, x_ref, l_ref, g_ref, o_ref):
        slot = iota((slots, rows), 0)
        expert = slot // capacity * n_head * n_pair + place_ref[0] * n_pair + place_ref[1]
        hits = jnp.zeros((slots, rows), F32)
        factor = jnp.zeros((slots, rows), F32)
        for k in range(top):
            same = l_ref[k : k + 1, :] == expert
            hits = jnp.where(same, 1.0, hits)
            factor = jnp.where(same, g_ref[k : k + 1, :], factor)
        earlier = (iota((rows, rows), 0) < iota((rows, rows), 1)).astype(F32).astype(BF16)
        rank = dot(hits.astype(BF16), earlier)
        factor = jnp.where(rank == (slot % capacity).astype(F32), factor, 0.0)
        x = x_ref[...].reshape(slots, width)
        out = jnp.zeros((rows, width), F32)
        for piece in pieces(factor):
            out = out + lax.dot_general(
                piece.astype(BF16), x, (((0,), (0,)), ((), ())), preferred_element_type=F32
            )
        o_ref[...] = out.reshape(n_head * n_pair, rows_own, width)

    return pl.pallas_call(
        kernel,
        in_specs=[SMEM, VMEM, VMEM, VMEM],
        out_shape=jax.ShapeDtypeStruct((n_head * n_pair, rows_own, width), F32),
        compiler_params=pltpu.CompilerParams(vmem_limit_bytes=LIMIT),
        name="weigh",
    )(place, returned, lists, weights)


def finish(own, shares):
    rows_own = shares.shape[1]

    def kernel(h_ref, x_ref, o_ref):
        o_ref[...] = (h_ref[0:rows_own, :] + jnp.sum(x_ref[...], axis=0)).astype(BF16)

    return pl.pallas_call(
        kernel,
        out_shape=jax.ShapeDtypeStruct(shares.shape[1:], BF16),
        compiler_params=pltpu.CompilerParams(vmem_limit_bytes=LIMIT),
        name="finish",
    )(own, shares)


def body(
    queries,
    prompt_keys,
    prompt_values,
    residual,
    out_weight,
    norm_gain,
    expert_lists,
    gate_weights,
    gate_up,
    down_proj,
):
    n_ctx = lax.axis_size("ctx")
    n_head = lax.axis_size("head")
    n_pair = lax.axis_size("pair")
    rows_own, width = residual.shape
    rows_all, heads, head_size = queries.shape
    block_rows, top = expert_lists.shape
    capacity = 2
    rows_half = n_head * rows_own
    pairs_block = rows_half * heads
    sizes = (n_ctx, n_head, n_pair, rows_own, top, capacity)
    head, pair = lax.axis_index("head"), lax.axis_index("pair")
    place = jnp.stack([head, pair]).astype(jnp.int32)

    units = queries.reshape(n_ctx * n_head, n_pair, rows_own * heads, head_size)
    keys = prompt_keys.reshape(-1, head_size)
    values = prompt_values.reshape(-1, head_size)
    theirs = attend_half((1 - pair).reshape(1), units, keys, values, n_ctx, pairs_block)
    swapped = lax.ppermute(theirs, "pair", [(0, 1), (1, 0)])
    ours = attend_half(pair.reshape(1), units, keys, values, n_ctx, pairs_block)
    lists, weights = expert_lists.T, gate_weights.T
    merged = merge_pair(ours, swapped, residual, lists)
    parts = lax.all_to_all(merged, "ctx", 0, 0, tiled=True)
    copies = combine_all(parts, rows_half, heads)
    picks, owns, weight_here = selection(parts, place, sizes, (out_weight,))
    attended = lax.all_to_all(copies, "ctx", 0, 0, tiled=True)
    attended, picks, owns = lax.optimization_barrier((attended, picks, owns))
    partial = project(attended, weight_here, parts, place, rows_half, heads, n_head * n_pair)
    partials = lax.all_to_all(partial, ("head", "pair"), 0, 0, tiled=True)
    sending = dispatch(partials, picks, owns, n_ctx, n_head, n_pair)
    arrived = lax.all_to_all(sending, "ctx", 0, 0, tiled=True)
    produced, own = run_expert(arrived, norm_gain, gate_up[0], down_proj[0], capacity)
    returned = lax.all_to_all(produced, "ctx", 0, 0, tiled=True)
    weighted = weigh(returned, lists, weights, place, sizes)
    shares = lax.all_to_all(weighted, ("head", "pair"), 0, 0, tiled=True)
    return finish(own, shares)


def solution(mesh):
    in_specs = (
        P("groups", "head", None),
        P(("groups", "ctx", "pair"), "head", None),
        P(("groups", "ctx", "pair"), "head", None),
        P(("groups", "ctx", "head", "pair"), None),
        P("head", "ctx"),
        P(),
        P(("groups", "ctx"), None),
        P(("groups", "ctx"), None),
        P(("ctx", "head", "pair"), None, None),
        P(("ctx", "head", "pair"), None, None),
    )
    out_specs = P(("groups", "ctx", "head", "pair"), None)
    return jax.shard_map(body, mesh=mesh, in_specs=in_specs, out_specs=out_specs, check_vma=False)
```

```python
import math

import jax
import jax.numpy as jnp
from jax import lax
from jax.experimental import pallas as pl
from jax.experimental.pallas import tpu as pltpu
from jax.sharding import PartitionSpec as P

F32 = jnp.float32
BF16 = jnp.bfloat16
LIMIT = 16 << 20
LOG2E = math.log2(math.e)
STATS = 8


SMEM = pl.BlockSpec(memory_space=pltpu.SMEM)
VMEM = pl.BlockSpec(memory_space=pltpu.VMEM)
HBM = pl.BlockSpec(memory_space=pltpu.HBM)


def in_hbm(x):
    return pltpu.with_memory_space_constraint(x, pltpu.HBM)


def iota(shape, dim):
    return lax.broadcasted_iota(jnp.int32, shape, dim)


def dot(a, b):
    return lax.dot_general(a, b, (((1,), (0,)), ((), ())), preferred_element_type=F32)


def as_row(column, lanes):
    n = column.shape[0]
    here = iota((n, lanes), 0) == iota((n, lanes), 1)
    return jnp.sum(jnp.where(here, jnp.broadcast_to(column, (n, lanes)), 0.0), axis=0, keepdims=True)


def as_column(row, n):
    lanes = row.shape[1]
    here = iota((n, lanes), 0) == iota((n, lanes), 1)
    return jnp.sum(jnp.where(here, jnp.broadcast_to(row, (n, lanes)), 0.0), axis=1, keepdims=True)


def pieces(row):
    first = row.astype(BF16).astype(F32)
    second = (row - first).astype(BF16).astype(F32)
    third = row - first - second
    return first, second, third


def stacked(rows, lanes):
    at = iota((STATS, lanes), 0)
    out = jnp.zeros((STATS, lanes), F32)
    for i, row in enumerate(rows):
        out = jnp.where(at == i, jnp.broadcast_to(row, (STATS, lanes)), out)
    return out


def attend_tiles(q_ref, k_ref, v_ref, o_ref, score_refs, tile_units, tile_blocks, pairs_block, ready):
    units, unit, width = q_ref.shape
    tile = tile_units * unit
    steps = units // tile_units
    scale = LOG2E / math.sqrt(width)

    def scores(i):
        q = q_ref[i * tile_units : (i + 1) * tile_units].reshape(tile, width)
        score_refs[i % 2][...] = lax.dot_general(
            q, k_ref[...], (((1,), (1,)), ((), ())), preferred_element_type=F32
        )

    scores(0)
    ready()
    for i in range(steps):
        if i + 1 < steps:
            scores(i + 1)
        here = score_refs[i % 2][...]
        top = jnp.max(here, axis=1, keepdims=True)
        probs = jnp.exp2((here - top) * scale)
        total = jnp.sum(probs, axis=1, keepdims=True)
        out = dot(probs.astype(BF16), v_ref[...]) / total
        level = top * scale + jnp.log(total) * LOG2E
        for b in range(tile_blocks):
            part = slice(b * pairs_block, (b + 1) * pairs_block)
            at = i * tile_blocks + b
            o_ref[at, 0:pairs_block, :] = out[part].astype(BF16)
            row = as_row(level[part], width)
            o_ref[at, pairs_block : pairs_block + STATS, :] = stacked(pieces(row), width).astype(BF16)


def attend(pair, queries, keys, values, blocks, pairs_block):
    units, _, unit, width = queries.shape
    length = keys.shape[0]
    tile_blocks = max(1, 256 // pairs_block)
    tile_units = tile_blocks * units // blocks
    out_shape = jax.ShapeDtypeStruct((blocks, pairs_block + STATS, width), BF16)
    scores = [pltpu.VMEM((tile_units * unit, length), F32)] * 2
    params = pltpu.CompilerParams(vmem_limit_bytes=24 << 20)

    def first(pair_ref, q_hbm, k_hbm, v_hbm, o_ref, q_own, k_ref, v_ref, q_ref, score_a, score_b, sems):
        copy_k = pltpu.make_async_copy(k_hbm, k_ref, sems.at[0])
        copy_q = pltpu.make_async_copy(q_hbm.at[:, 1 - pair_ref[0]], q_ref, sems.at[1])
        copy_v = pltpu.make_async_copy(v_hbm, v_ref, sems.at[2])
        copy_own = pltpu.make_async_copy(q_hbm.at[:, pair_ref[0]], q_own, sems.at[3])
        copy_q.start()
        copy_k.start()
        copy_v.start()
        copy_own.start()
        copy_q.wait()
        copy_k.wait()
        attend_tiles(
            q_ref, k_ref, v_ref, o_ref, (score_a, score_b), tile_units, tile_blocks, pairs_block, copy_v.wait
        )
        copy_own.wait()

    def second(q_ref, k_ref, v_ref, o_ref, score_a, score_b):
        attend_tiles(
            q_ref, k_ref, v_ref, o_ref, (score_a, score_b), tile_units, tile_blocks, pairs_block, lambda: None
        )

    theirs, q_own, k_here, v_here = pl.pallas_call(
        first,
        in_specs=[SMEM, HBM, HBM, HBM],
        out_specs=[VMEM] * 4,
        out_shape=[
            out_shape,
            jax.ShapeDtypeStruct((units, unit, width), BF16),
            jax.ShapeDtypeStruct(keys.shape, BF16),
            jax.ShapeDtypeStruct(values.shape, BF16),
        ],
        scratch_shapes=[pltpu.VMEM((units, unit, width), BF16), *scores, pltpu.SemaphoreType.DMA((4,))],
        compiler_params=params,
        name="attend_theirs",
    )(pair.reshape(1), in_hbm(queries), in_hbm(keys), in_hbm(values))
    swapped = lax.ppermute(theirs, "pair", [(0, 1), (1, 0)])
    ours = pl.pallas_call(
        second,
        in_specs=[VMEM] * 3,
        out_specs=VMEM,
        out_shape=out_shape,
        scratch_shapes=scores,
        compiler_params=params,
        name="attend_ours",
    )(q_own, k_here, v_here)
    return ours, swapped


def levels_of(ref, pairs_block):
    stats = ref[:, pairs_block : pairs_block + STATS, :].astype(F32)
    return stats[:, 0, :] + stats[:, 1, :] + stats[:, 2, :]


def merge_pair(mine, other, residual, names, weights):
    blocks, height, width = mine.shape
    pairs_block = height - STATS

    def kernel(a_ref, b_ref, r_hbm, n_hbm, g_hbm, o_ref, r_ref, n_ref, g_ref, sems):
        copy_r = pltpu.make_async_copy(r_hbm, r_ref, sems.at[0])
        copy_n = pltpu.make_async_copy(n_hbm, n_ref, sems.at[1])
        copy_g = pltpu.make_async_copy(g_hbm, g_ref, sems.at[2])
        copy_r.start()
        copy_n.start()
        copy_g.start()
        level_a, level_b = levels_of(a_ref, pairs_block), levels_of(b_ref, pairs_block)
        highest = jnp.maximum(level_a, level_b)
        share_a, share_b = jnp.exp2(level_a - highest), jnp.exp2(level_b - highest)
        total = share_a + share_b
        share_a, share_b = share_a / total, share_b / total
        level = highest + jnp.log(total) * LOG2E
        first, second, third = pieces(level)
        for b in range(blocks):
            col_a, col_b = as_column(share_a[b : b + 1], pairs_block), as_column(share_b[b : b + 1], pairs_block)
            both = a_ref[b, 0:pairs_block, :].astype(F32) * col_a + b_ref[b, 0:pairs_block, :].astype(F32) * col_b
            o_ref[b, 0:pairs_block, :] = both.astype(BF16)
        copy_r.wait()
        copy_n.wait()
        copy_g.wait()
        residual_all = r_ref[...].astype(F32)
        top, rows = n_ref.shape
        spread = (iota((rows, width), 1) % rows == iota((rows, width), 0)).astype(F32).astype(BF16)
        kept = iota((top, width), 1) // rows == iota((top, width), 0)

        def in_lanes(table):
            return jnp.sum(jnp.where(kept, dot(table.astype(BF16), spread), 0.0), axis=0, keepdims=True)

        listed = in_lanes(n_ref[...].astype(F32))
        gates = g_ref[...]
        rounded = gates.astype(BF16).astype(F32)
        gate_first, gate_second = in_lanes(rounded), in_lanes(gates - rounded)
        for b in range(blocks):
            own = residual_all[:, b * width : (b + 1) * width]
            rows_b = (first[b : b + 1], second[b : b + 1], third[b : b + 1], own[0:1], own[1:2], listed)
            rows_b = rows_b + (gate_first, gate_second)
            o_ref[b, pairs_block:height, :] = stacked(rows_b, width).astype(BF16)

    return pl.pallas_call(
        kernel,
        in_specs=[VMEM, VMEM, HBM, HBM, HBM],
        out_shape=jax.ShapeDtypeStruct((blocks, height, width), BF16),
        scratch_shapes=[
            pltpu.VMEM(residual.shape, residual.dtype),
            pltpu.VMEM(names.shape, names.dtype),
            pltpu.VMEM(weights.shape, weights.dtype),
            pltpu.SemaphoreType.DMA((3,)),
        ],
        compiler_params=pltpu.CompilerParams(vmem_limit_bytes=LIMIT),
        name="merge_pair",
    )(mine, other, in_hbm(residual), in_hbm(names), in_hbm(weights))


def combine_all(parts, rows_half, heads):
    sources, height, width = parts.shape
    pairs_block = height - STATS

    def kernel(x_ref, o_hbm, acc_ref, att_ref, sem):
        level = levels_of(x_ref, pairs_block)
        share = jnp.exp2(level - jnp.max(level, axis=0, keepdims=True))
        share = share / jnp.sum(share, axis=0, keepdims=True)
        acc = jnp.zeros((pairs_block, width), F32)
        for s in range(sources):
            acc = acc + x_ref[s, 0:pairs_block, :].astype(F32) * as_column(share[s : s + 1], pairs_block)
        acc_ref[...] = acc
        by_head = [acc_ref[pl.ds(h, rows_half, stride=heads), :] for h in range(heads)]
        att_ref[...] = jnp.concatenate(by_head, axis=0).astype(BF16)
        copies = [pltpu.make_async_copy(att_ref, o_hbm.at[s], sem.at[s]) for s in range(sources)]
        for copy in copies:
            copy.start()
        for copy in copies:
            copy.wait()

    return pl.pallas_call(
        kernel,
        in_specs=[VMEM],
        out_specs=HBM,
        out_shape=pltpu.HBM((sources, pairs_block, width), BF16),
        scratch_shapes=[
            pltpu.VMEM((pairs_block, width), F32),
            pltpu.VMEM((pairs_block, width), BF16),
            pltpu.SemaphoreType.DMA((sources,)),
        ],
        compiler_params=pltpu.CompilerParams(vmem_limit_bytes=LIMIT),
        name="combine_all",
    )(parts)


def project(attended, weight, parts, place, rows_half, heads, copies):
    blocks, pairs_block, width = attended.shape
    columns = weight.shape[1]
    rows = blocks * rows_half

    def kernel(place_ref, a_ref, w_ref, s_ref, o_ref):
        a = a_ref[...].astype(F32)
        by_head = [a[:, h * rows_half : (h + 1) * rows_half, :].reshape(rows, width) for h in range(heads)]
        out = dot(jnp.concatenate(by_head, axis=1).astype(BF16), w_ref[...])
        out = out.reshape(blocks, rows_half, columns)
        stats = s_ref[:, pairs_block : pairs_block + STATS, :].astype(F32)
        at = iota((blocks, rows_half, columns), 1)
        first = 2 * place_ref[0]
        out = out + jnp.where(at == first, stats[:, 3:4, :], 0.0) + jnp.where(at == first + 1, stats[:, 4:5, :], 0.0)
        out = out.reshape(rows, columns).astype(BF16)
        for i in range(copies):
            o_ref[i] = out

    return pl.pallas_call(
        kernel,
        in_specs=[SMEM, VMEM, VMEM, VMEM],
        out_shape=jax.ShapeDtypeStruct((copies, rows, columns), BF16),
        compiler_params=pltpu.CompilerParams(vmem_limit_bytes=LIMIT),
        name="project",
    )(place, attended, weight, parts)


def selection(parts, place, sizes, fetched):
    n_ctx, n_head, n_pair, rows_own, top, capacity = sizes
    block_rows = n_head * n_pair * rows_own
    rows_all = n_ctx * block_rows
    blocks, height, width = parts.shape
    per_peer = n_ctx * capacity

    def natural(lane):
        pair = lane // (rows_all // n_pair)
        rest = lane % (rows_all // n_pair)
        block = rest // (n_head * rows_own)
        head = (rest // rows_own) % n_head
        return block, (head * n_pair + pair) * rows_own + rest % rows_own

    count_fetched = len(fetched)

    def kernel(place_ref, s_ref, *refs):
        sources, d_ref, o_ref = refs[:count_fetched], refs[count_fetched], refs[count_fetched + 1]
        targets, sems = refs[count_fetched + 2 : -1], refs[-1]
        fetches = [pltpu.make_async_copy(a, b, sems.at[i]) for i, (a, b) in enumerate(zip(sources, targets))]
        for fetch in fetches:
            fetch.start()
        stats = s_ref[:, height - STATS : height, :].astype(F32)
        listed = stats[:, 5, :]
        count = n_ctx * n_ctx
        repeated = jnp.concatenate([listed] * n_ctx, axis=0)
        expert = (iota((count, width), 0) // n_ctx * n_head * n_pair + place_ref[0] * n_pair + place_ref[1]).astype(F32)
        equal = (repeated == expert).astype(F32).astype(BF16)
        fold = (iota((width, block_rows), 0) % block_rows == iota((width, block_rows), 1)).astype(F32).astype(BF16)
        hits = dot(equal, fold)
        earlier = (iota((block_rows, block_rows), 0) < iota((block_rows, block_rows), 1)).astype(F32).astype(BF16)
        rank = dot(hits.astype(BF16), earlier)
        slot = jnp.where(hits > 0.5, rank + 1.0, 0.0).astype(BF16)
        expand = iota((count * capacity, count), 0) // capacity == iota((count * capacity, count), 1)
        slot = dot(expand.astype(F32).astype(BF16), slot).astype(BF16)
        block, row = natural(iota((block_rows, rows_all), 1))
        spread = (iota((block_rows, rows_all), 0) == row).astype(F32).astype(BF16)
        slot = dot(slot, spread)
        at = iota((count * capacity, rows_all), 0)
        block, row = natural(iota((count * capacity, rows_all), 1))
        mine = (block == (at // capacity) % n_ctx) & (slot == (at % capacity + 1).astype(F32))
        d_ref[...] = mine.astype(F32).astype(BF16)
        own = (place_ref[2] * n_head * n_pair + place_ref[0] * n_pair + place_ref[1]).astype(F32)
        same = (listed == own).astype(F32).astype(BF16)
        rank = dot(dot(same, fold).astype(BF16), earlier).astype(BF16)
        back = (iota((block_rows, width), 1) % block_rows == iota((block_rows, width), 0)).astype(F32).astype(BF16)
        twice = iota((per_peer, n_ctx), 0) // capacity == iota((per_peer, n_ctx), 1)
        twice = twice.astype(F32).astype(BF16)
        rank = dot(twice, dot(rank, back).astype(BF16))
        used = (dot(twice, same) > 0.5) & (rank == (iota((per_peer, width), 0) % capacity).astype(F32))
        gates = dot(twice, stats[:, 6, :].astype(BF16)) + dot(twice, stats[:, 7, :].astype(BF16))
        gate = jnp.sum(jnp.where(used, gates, 0.0), axis=1, keepdims=True)
        is_first = used & (iota((per_peer, width), 1) < block_rows)
        is_first = jnp.sum(jnp.where(is_first, 1.0, 0.0), axis=1, keepdims=True)
        o_ref[...] = jnp.where(iota((per_peer, width), 1) == 0, gate, is_first)
        for fetch in fetches:
            fetch.wait()

    return pl.pallas_call(
        kernel,
        in_specs=[SMEM, VMEM] + [HBM] * count_fetched,
        out_specs=[VMEM] * (2 + count_fetched),
        out_shape=[
            jax.ShapeDtypeStruct((n_ctx * per_peer, rows_all), BF16),
            jax.ShapeDtypeStruct((per_peer, width), F32),
        ]
        + [jax.ShapeDtypeStruct(x.shape, x.dtype) for x in fetched],
        scratch_shapes=[pltpu.SemaphoreType.DMA((count_fetched,))],
        compiler_params=pltpu.CompilerParams(vmem_limit_bytes=LIMIT),
        name="selection",
    )(place, parts, *[in_hbm(x) for x in fetched])


def dispatch(partials, picks, n_ctx, n_head, n_pair):
    copies, rows, columns = partials.shape
    per_peer = picks.shape[0] // n_ctx

    def kernel(x_ref, d_ref, o_ref):
        halves = []
        for p in range(n_pair):
            acc = x_ref[p].astype(F32)
            for h in range(1, n_head):
                acc = acc + x_ref[h * n_pair + p].astype(F32)
            halves.append(acc)
        hidden = jnp.concatenate(halves, axis=0).astype(BF16)
        o_ref[...] = dot(d_ref[...], hidden).reshape(n_ctx, per_peer, columns).astype(BF16)

    return pl.pallas_call(
        kernel,
        out_shape=jax.ShapeDtypeStruct((n_ctx, per_peer, columns), BF16),
        compiler_params=pltpu.CompilerParams(vmem_limit_bytes=LIMIT),
        name="dispatch",
    )(partials, picks)


def run_expert(parts, slot_facts, gain, gate_up, down, capacity):
    sources, slots, columns = parts.shape
    width = sources * columns
    units = down.shape[0]
    chunks = 8
    chunk = width // chunks

    def kernel(x_ref, f_ref, g_ref, up_hbm, down_hbm, y_ref, up_ref, down_ref, sems):
        ups = [
            pltpu.make_async_copy(
                up_hbm.at[pl.ds(i * chunk, chunk)], up_ref.at[pl.ds(i * chunk, chunk)], sems.at[i]
            )
            for i in range(chunks)
        ]
        last = pltpu.make_async_copy(down_hbm, down_ref, sems.at[chunks])
        for copy in ups:
            copy.start()
        last.start()
        rows = jnp.concatenate([x_ref[s].astype(F32) for s in range(sources)], axis=1)
        mean = jnp.sum(rows * rows, axis=1, keepdims=True) * (1.0 / width)
        normed = (rows * lax.rsqrt(mean + 1e-06) * g_ref[...]).astype(BF16)
        both = jnp.zeros((slots, 2 * units), F32)
        for i in range(chunks):
            ups[i].wait()
            both = both + dot(normed[:, i * chunk : (i + 1) * chunk], up_ref[i * chunk : (i + 1) * chunk, :])
        gate = both[:, :units]
        inner = (gate / (1.0 + jnp.exp(-gate)) * both[:, units:]).astype(BF16)
        last.wait()
        out = dot(inner, down_ref[...]) * f_ref[:, 0:1] + rows * f_ref[:, 1:2]
        y_ref[...] = out.astype(BF16).reshape(sources, capacity, width)

    return pl.pallas_call(
        kernel,
        in_specs=[VMEM, VMEM, VMEM, HBM, HBM],
        out_shape=jax.ShapeDtypeStruct((sources, capacity, width), BF16),
        scratch_shapes=[
            pltpu.VMEM(gate_up.shape, BF16),
            pltpu.VMEM(down.shape, BF16),
            pltpu.SemaphoreType.DMA((chunks + 1,)),
        ],
        compiler_params=pltpu.CompilerParams(vmem_limit_bytes=24 << 20),
        name="run_expert",
    )(parts, slot_facts, gain.reshape(1, width), in_hbm(gate_up), in_hbm(down))


def sum_rows(returned, lists, place, sizes):
    n_ctx, n_head, n_pair, rows_own, top, capacity = sizes
    slots, width = n_ctx * capacity, returned.shape[2]
    rows = lists.shape[1]

    def kernel(place_ref, x_ref, l_ref, o_ref):
        slot = iota((slots, rows), 0)
        expert = slot // capacity * n_head * n_pair + place_ref[0] * n_pair + place_ref[1]
        hits = jnp.zeros((slots, rows), F32)
        for k in range(top):
            hits = jnp.where(l_ref[k : k + 1, :] == expert, 1.0, hits)
        earlier = (iota((rows, rows), 0) < iota((rows, rows), 1)).astype(F32).astype(BF16)
        rank = dot(hits.astype(BF16), earlier)
        taken = jnp.where(rank == (slot % capacity).astype(F32), hits, 0.0).astype(BF16)
        x = x_ref[...].reshape(slots, width)
        out = lax.dot_general(taken, x, (((0,), (0,)), ((), ())), preferred_element_type=F32)
        o_ref[...] = out.reshape(n_head * n_pair, rows_own, width)

    return pl.pallas_call(
        kernel,
        in_specs=[SMEM, VMEM, VMEM],
        out_shape=jax.ShapeDtypeStruct((n_head * n_pair, rows_own, width), F32),
        compiler_params=pltpu.CompilerParams(vmem_limit_bytes=LIMIT),
        name="sum_rows",
    )(place, returned, lists)


def finish(shares):
    def kernel(x_ref, o_ref):
        o_ref[...] = jnp.sum(x_ref[...], axis=0).astype(BF16)

    return pl.pallas_call(
        kernel,
        out_shape=jax.ShapeDtypeStruct(shares.shape[1:], BF16),
        compiler_params=pltpu.CompilerParams(vmem_limit_bytes=LIMIT),
        name="finish",
    )(shares)


def body(
    queries,
    prompt_keys,
    prompt_values,
    residual,
    out_weight,
    norm_gain,
    expert_lists,
    gate_weights,
    gate_up,
    down_proj,
):
    n_ctx = lax.axis_size("ctx")
    n_head = lax.axis_size("head")
    n_pair = lax.axis_size("pair")
    rows_own, width = residual.shape
    rows_all, heads, head_size = queries.shape
    block_rows, top = expert_lists.shape
    capacity = 2
    rows_half = n_head * rows_own
    pairs_block = rows_half * heads
    sizes = (n_ctx, n_head, n_pair, rows_own, top, capacity)
    head, pair = lax.axis_index("head"), lax.axis_index("pair")
    place = jnp.stack([head, pair, lax.axis_index("ctx")]).astype(jnp.int32)

    units = queries.reshape(n_ctx * n_head, n_pair, rows_own * heads, head_size)
    keys = prompt_keys.reshape(-1, head_size)
    values = prompt_values.reshape(-1, head_size)
    ours, swapped = attend(pair, units, keys, values, n_ctx, pairs_block)
    lists, weights = expert_lists.T, gate_weights.T
    merged = merge_pair(ours, swapped, residual, lists, weights)
    parts = lax.all_to_all(merged, "ctx", 0, 0, tiled=True)
    copies = combine_all(parts, rows_half, heads)
    picks, slot_facts, weight_here = selection(parts, place, sizes, (out_weight,))
    attended = lax.all_to_all(copies, "ctx", 0, 0, tiled=True)
    attended, picks, slot_facts = lax.optimization_barrier((attended, picks, slot_facts))
    partial = project(attended, weight_here, parts, place, rows_half, heads, n_head * n_pair)
    partials = lax.all_to_all(partial, ("head", "pair"), 0, 0, tiled=True)
    sending = dispatch(partials, picks, n_ctx, n_head, n_pair)
    arrived = lax.all_to_all(sending, "ctx", 0, 0, tiled=True)
    produced = run_expert(arrived, slot_facts, norm_gain, gate_up[0], down_proj[0], capacity)
    returned = lax.all_to_all(produced, "ctx", 0, 0, tiled=True)
    weighted = sum_rows(returned, lists, place, sizes)
    shares = lax.all_to_all(weighted, ("head", "pair"), 0, 0, tiled=True)
    return finish(shares)


def solution(mesh):
    in_specs = (
        P("groups", "head", None),
        P(("groups", "ctx", "pair"), "head", None),
        P(("groups", "ctx", "pair"), "head", None),
        P(("groups", "ctx", "head", "pair"), None),
        P("head", "ctx"),
        P(),
        P(("groups", "ctx"), None),
        P(("groups", "ctx"), None),
        P(("ctx", "head", "pair"), None, None),
        P(("ctx", "head", "pair"), None, None),
    )
    out_specs = P(("groups", "ctx", "head", "pair"), None)
    return jax.shard_map(body, mesh=mesh, in_specs=in_specs, out_specs=out_specs, check_vma=False)
```

```python
import functools
import math

import jax
import jax.numpy as jnp
from jax import lax
from jax.experimental import pallas as pl
from jax.experimental.pallas import tpu as pltpu
from jax.sharding import PartitionSpec as P


F32 = jnp.float32
BF16 = jnp.bfloat16
LIMIT = 16 << 20
LOG2E = math.log2(math.e)
STATS = 8


SMEM = pl.BlockSpec(memory_space=pltpu.SMEM)
VMEM = pl.BlockSpec(memory_space=pltpu.VMEM)
HBM = pl.BlockSpec(memory_space=pltpu.HBM)


def in_hbm(x):
    return pltpu.with_memory_space_constraint(x, pltpu.HBM)


def iota(shape, dim):
    return lax.broadcasted_iota(jnp.int32, shape, dim)


def dot(a, b):
    return lax.dot_general(a, b, (((1,), (0,)), ((), ())), preferred_element_type=F32)


def as_row(column, lanes):
    n = column.shape[0]
    here = iota((n, lanes), 0) == iota((n, lanes), 1)
    return jnp.sum(jnp.where(here, jnp.broadcast_to(column, (n, lanes)), 0.0), axis=0, keepdims=True)


def as_column(row, n):
    lanes = row.shape[1]
    here = iota((n, lanes), 0) == iota((n, lanes), 1)
    return jnp.sum(jnp.where(here, jnp.broadcast_to(row, (n, lanes)), 0.0), axis=1, keepdims=True)


def pieces(row):
    first = row.astype(BF16).astype(F32)
    second = (row - first).astype(BF16).astype(F32)
    third = row - first - second
    return first, second, third


def stacked(rows, lanes):
    at = iota((STATS, lanes), 0)
    out = jnp.zeros((STATS, lanes), F32)
    for i, row in enumerate(rows):
        out = jnp.where(at == i, jnp.broadcast_to(row, (STATS, lanes)), out)
    return out


def attend_tiles(q_ref, k_ref, v_ref, o_ref, score_refs, pairs_block, ready):
    blocks, _, _, width = q_ref.shape
    tile_blocks = max(1, 128 // pairs_block)
    tile = tile_blocks * pairs_block
    steps = blocks // tile_blocks
    scale = LOG2E / math.sqrt(width)

    def scores(i):
        q = q_ref[i * tile_blocks : (i + 1) * tile_blocks].reshape(tile, width)
        score_refs[i % 2][...] = lax.dot_general(
            q, k_ref[...], (((1,), (1,)), ((), ())), preferred_element_type=F32
        )

    scores(0)
    ready()
    for i in range(steps):
        if i + 1 < steps:
            scores(i + 1)
        here = score_refs[i % 2][...]
        top = jnp.max(here, axis=1, keepdims=True)
        probs = jnp.exp2((here - top) * scale)
        total = jnp.sum(probs, axis=1, keepdims=True)
        out = dot(probs.astype(BF16), v_ref[...]) / total
        level = top * scale + jnp.log(total) * LOG2E
        for b in range(tile_blocks):
            part = slice(b * pairs_block, (b + 1) * pairs_block)
            at = i * tile_blocks + b
            o_ref[at, 0:pairs_block, :] = out[part].astype(BF16)
            row = as_row(level[part], width)
            o_ref[at, pairs_block : pairs_block + STATS, :] = stacked(pieces(row), width).astype(BF16)


def attend_first(place, queries, keys, values, residual, names, weights, pairs_block):
    blocks, _, n_head, _, unit, width = queries.shape
    length = keys.shape[0]
    quarter = (blocks, n_head, unit, width)
    tile = max(1, 128 // pairs_block) * pairs_block

    def kernel(
        place_ref, q_hbm, k_hbm, v_hbm, r_hbm, n_hbm, g_hbm,
        o_ref, q2, q3, q4, k_ref, v_ref, r_ref, facts_ref,
        q1, score_a, score_b, n_ref, g_ref, sems,
    ):
        pair, parity = place_ref[1], place_ref[3]
        small = [
            pltpu.make_async_copy(a, b, sems.at[6 + i])
            for i, (a, b) in enumerate(((r_hbm, r_ref), (n_hbm, n_ref), (g_hbm, g_ref)))
        ]
        copy_k = pltpu.make_async_copy(k_hbm, k_ref, sems.at[0])
        copy_v = pltpu.make_async_copy(v_hbm, v_ref, sems.at[1])
        choices = ((q1, 1 - parity, 1 - pair), (q2, 1 - parity, pair), (q3, parity, 1 - pair), (q4, parity, pair))
        copies = [
            pltpu.make_async_copy(q_hbm.at[:, side, :, core], ref, sems.at[2 + i])
            for i, (ref, side, core) in enumerate(choices)
        ]
        for copy in small:
            copy.start()
        copies[0].start()
        copy_k.start()
        copy_v.start()
        for copy in copies[1:]:
            copy.start()
        for copy in small:
            copy.wait()
        top, rows = n_ref.shape
        spread = (iota((rows, width), 1) % rows == iota((rows, width), 0)).astype(F32).astype(BF16)
        kept = iota((top, width), 1) // rows == iota((top, width), 0)

        def in_lanes(table):
            return jnp.sum(jnp.where(kept, dot(table.astype(BF16), spread), 0.0), axis=0, keepdims=True)

        gates = g_ref[...]
        rounded = gates.astype(BF16).astype(F32)
        facts = (in_lanes(n_ref[...].astype(F32)), in_lanes(rounded), in_lanes(gates - rounded))
        facts_ref[...] = stacked(facts, width)
        copies[0].wait()
        copy_k.wait()
        attend_tiles(q1, k_ref, v_ref, o_ref, (score_a, score_b), pairs_block, copy_v.wait)
        for copy in copies[1:]:
            copy.wait()

    return pl.pallas_call(
        kernel,
        in_specs=[SMEM] + [HBM] * 6,
        out_specs=[VMEM] * 8,
        out_shape=[jax.ShapeDtypeStruct((blocks, pairs_block + STATS, width), BF16)]
        + [jax.ShapeDtypeStruct(quarter, BF16)] * 3
        + [jax.ShapeDtypeStruct(x.shape, BF16) for x in (keys, values, residual)]
        + [jax.ShapeDtypeStruct((STATS, width), F32)],
        scratch_shapes=[pltpu.VMEM(quarter, BF16)]
        + [pltpu.VMEM((tile, length), F32)] * 2
        + [pltpu.VMEM(names.shape, names.dtype), pltpu.VMEM(weights.shape, weights.dtype)]
        + [pltpu.SemaphoreType.DMA((9,))],
        compiler_params=pltpu.CompilerParams(vmem_limit_bytes=LIMIT),
        name="attend_first",
    )(place, *[in_hbm(x) for x in (queries, keys, values, residual, names, weights)])


def attend_next(queries, keys, values, pairs_block):
    blocks, _, _, width = queries.shape
    tile = max(1, 128 // pairs_block) * pairs_block

    def kernel(q_ref, k_ref, v_ref, o_ref, score_a, score_b):
        attend_tiles(q_ref, k_ref, v_ref, o_ref, (score_a, score_b), pairs_block, lambda: None)

    return pl.pallas_call(
        kernel,
        in_specs=[VMEM] * 3,
        out_shape=jax.ShapeDtypeStruct((blocks, pairs_block + STATS, width), BF16),
        scratch_shapes=[pltpu.VMEM((tile, keys.shape[0]), F32)] * 2,
        compiler_params=pltpu.CompilerParams(vmem_limit_bytes=LIMIT),
        name="attend_next",
    )(queries, keys, values)


def levels_of(ref, pairs_block):
    stats = ref[:, pairs_block : pairs_block + STATS, :].astype(F32)
    return stats[:, 0, :] + stats[:, 1, :] + stats[:, 2, :]


def merge(partials, residual, facts, place, theirs):
    count = len(partials)
    blocks, height, width = partials[0].shape
    pairs_block = height - STATS
    height_out = height + STATS * (count - 2)

    def kernel(place_ref, *refs):
        parts, (r_ref, f_ref, o_ref) = refs[:count], refs[count:]
        levels = [levels_of(ref, pairs_block) for ref in parts]
        highest = functools.reduce(jnp.maximum, levels)
        shares = [jnp.exp2(level - highest) for level in levels]
        total = functools.reduce(jnp.add, shares)
        shares = [share / total for share in shares]
        first, second, third = pieces(highest + jnp.log(total) * LOG2E)
        for b in range(blocks):
            merged = jnp.zeros((pairs_block, width), F32)
            for ref, share in zip(parts, shares):
                merged = merged + ref[b, 0:pairs_block, :].astype(F32) * as_column(share[b : b + 1], pairs_block)
            o_ref[b, 0:pairs_block, :] = merged.astype(BF16)
        residual_all = r_ref[...].astype(F32)
        facts = tuple(f_ref[i : i + 1, :] for i in range(3))
        side = 1 - place_ref[3] if theirs else place_ref[3]
        for b in range(blocks):
            even = residual_all[:, 2 * b * width : (2 * b + 1) * width]
            odd = residual_all[:, (2 * b + 1) * width : (2 * b + 2) * width]
            own = jnp.where(jnp.broadcast_to(side, even.shape) == 0, even, odd)
            rows_b = (first[b : b + 1], second[b : b + 1], third[b : b + 1], own[0:1], own[1:2])
            o_ref[b, pairs_block:height, :] = stacked(rows_b + facts, width).astype(BF16)
            for ref in parts[2:]:
                o_ref[b, height:height_out, :] = ref[b, pairs_block:height, :]

    return pl.pallas_call(
        kernel,
        in_specs=[SMEM] + [VMEM] * (count + 2),
        out_shape=jax.ShapeDtypeStruct((blocks, height_out, width), BF16),
        compiler_params=pltpu.CompilerParams(vmem_limit_bytes=LIMIT),
        name="merge",
    )(place, *partials, residual, facts)


def combine_all(parts, rows_half, heads, peers):
    sources, height, width = parts.shape
    pairs_block = height - 2 * STATS

    def kernel(x_ref, o_hbm, acc_ref, att_ref, sem):
        level = levels_of(x_ref, pairs_block)
        share = jnp.exp2(level - jnp.max(level, axis=0, keepdims=True))
        share = share / jnp.sum(share, axis=0, keepdims=True)
        acc = jnp.zeros((pairs_block, width), F32)
        for s in range(sources):
            acc = acc + x_ref[s, 0:pairs_block, :].astype(F32) * as_column(share[s : s + 1], pairs_block)
        acc_ref[...] = acc
        by_head = [acc_ref[pl.ds(h, rows_half, stride=heads), :] for h in range(heads)]
        att_ref[...] = jnp.concatenate(by_head, axis=0).astype(BF16)
        copies = [pltpu.make_async_copy(att_ref, o_hbm.at[s], sem.at[s]) for s in range(peers)]
        for copy in copies:
            copy.start()
        for copy in copies:
            copy.wait()

    return pl.pallas_call(
        kernel,
        in_specs=[VMEM],
        out_specs=HBM,
        out_shape=pltpu.HBM((peers, pairs_block, width), BF16),
        scratch_shapes=[
            pltpu.VMEM((pairs_block, width), F32),
            pltpu.VMEM((pairs_block, width), BF16),
            pltpu.SemaphoreType.DMA((peers,)),
        ],
        compiler_params=pltpu.CompilerParams(vmem_limit_bytes=LIMIT),
        name="combine_all",
    )(parts)


def project(attended, weight, parts, place, rows_half, heads, copies):
    blocks, pairs_block, width = attended.shape
    columns = weight.shape[1]
    rows = blocks * rows_half

    def kernel(place_ref, a_ref, w_ref, s_ref, o_ref):
        a = a_ref[...].astype(F32)
        by_head = [a[:, h * rows_half : (h + 1) * rows_half, :].reshape(rows, width) for h in range(heads)]
        out = dot(jnp.concatenate(by_head, axis=1).astype(BF16), w_ref[...])
        stats_all = s_ref[:, pairs_block : pairs_block + 2 * STATS, :].astype(F32)
        same, other = stats_all[:, :STATS], stats_all[:, STATS:]
        at = iota((rows_half, columns), 0)
        first = 2 * place_ref[0]
        crossed = jnp.broadcast_to(place_ref[3], (STATS, columns)).astype(F32)
        finished = []
        for block in range(blocks):
            one, two = same[block // 2], other[block // 2]
            share = 1.0 - crossed if block % 2 == 0 else crossed
            stats = one * share + two * (1.0 - share)
            added = jnp.where(at == first, stats[3:4], 0.0) + jnp.where(at == first + 1, stats[4:5], 0.0)
            finished.append(out[block * rows_half : (block + 1) * rows_half] + added)
        out = jnp.concatenate(finished, axis=0).astype(BF16)
        for i in range(copies):
            o_ref[i] = out

    return pl.pallas_call(
        kernel,
        in_specs=[SMEM, VMEM, VMEM, VMEM],
        out_shape=jax.ShapeDtypeStruct((copies, rows, columns), BF16),
        compiler_params=pltpu.CompilerParams(vmem_limit_bytes=LIMIT),
        name="project",
    )(place, attended, weight, parts)


def selection(parts, place, sizes, fetched):
    n_ctx, n_head, n_pair, rows_own, _, capacity = sizes
    block_rows = n_head * n_pair * rows_own
    rows_all = n_ctx * block_rows
    blocks, height, width = parts.shape
    per_peer = n_ctx * capacity

    def natural(lane):
        pair = lane // (rows_all // n_pair)
        rest = lane % (rows_all // n_pair)
        block = rest // (n_head * rows_own)
        head = (rest // rows_own) % n_head
        return block, (head * n_pair + pair) * rows_own + rest % rows_own

    count_fetched = len(fetched)

    def kernel(place_ref, s_ref, *refs):
        sources, d_ref, o_ref = refs[:count_fetched], refs[count_fetched], refs[count_fetched + 1]
        targets, sems = refs[count_fetched + 2 : -1], refs[-1]
        fetches = [
            pltpu.make_async_copy(a.at[:, pl.ds(0, b.shape[1])], b, sems.at[i])
            for i, (a, b) in enumerate(zip(sources, targets))
        ]
        for fetch in fetches:
            fetch.start()
        stats = s_ref[:, height - 2 * STATS : height, :].astype(F32)
        came = iota((n_ctx, n_ctx), 1)
        came = came % blocks * 2 + jnp.where(came < blocks, place_ref[3], 1 - place_ref[3])
        order = (came == iota((n_ctx, n_ctx), 0)).astype(F32).astype(BF16)

        def in_order(row):
            rows = jnp.concatenate([stats[:, row, :], stats[:, row + STATS, :]], axis=0)
            return dot(order, rows.astype(BF16))

        listed = in_order(5)
        count = n_ctx * n_ctx
        repeated = jnp.concatenate([listed] * n_ctx, axis=0)
        expert = (iota((count, width), 0) // n_ctx * n_head * n_pair + place_ref[0] * n_pair + place_ref[1]).astype(F32)
        equal = (repeated == expert).astype(F32).astype(BF16)
        fold = (iota((width, block_rows), 0) % block_rows == iota((width, block_rows), 1)).astype(F32).astype(BF16)
        hits = dot(equal, fold)
        earlier = (iota((block_rows, block_rows), 0) < iota((block_rows, block_rows), 1)).astype(F32).astype(BF16)
        rank = dot(hits.astype(BF16), earlier)
        slot = jnp.where(hits > 0.5, rank + 1.0, 0.0).astype(BF16)
        expand = iota((count * capacity, count), 0) // capacity == iota((count * capacity, count), 1)
        slot = dot(expand.astype(F32).astype(BF16), slot).astype(BF16)
        block, row = natural(iota((block_rows, rows_all), 1))
        spread = (iota((block_rows, rows_all), 0) == row).astype(F32).astype(BF16)
        slot = dot(slot, spread)
        at = iota((count * capacity, rows_all), 0)
        block, row = natural(iota((count * capacity, rows_all), 1))
        mine = (block == (at // capacity) % n_ctx) & (slot == (at % capacity + 1).astype(F32))
        d_ref[...] = mine.astype(F32).astype(BF16)
        own = (place_ref[2] * n_head * n_pair + place_ref[0] * n_pair + place_ref[1]).astype(F32)
        same = (listed == own).astype(F32).astype(BF16)
        rank = dot(dot(same, fold).astype(BF16), earlier).astype(BF16)
        back = (iota((block_rows, width), 1) % block_rows == iota((block_rows, width), 0)).astype(F32).astype(BF16)
        twice = iota((per_peer, n_ctx), 0) // capacity == iota((per_peer, n_ctx), 1)
        twice = twice.astype(F32).astype(BF16)
        rank = dot(twice, dot(rank, back).astype(BF16))
        used = (dot(twice, same) > 0.5) & (rank == (iota((per_peer, width), 0) % capacity).astype(F32))
        gates = dot(twice, in_order(6).astype(BF16)) + dot(twice, in_order(7).astype(BF16))
        gate = jnp.sum(jnp.where(used, gates, 0.0), axis=1, keepdims=True)
        is_first = used & (iota((per_peer, width), 1) < block_rows)
        is_first = jnp.sum(jnp.where(is_first, 1.0, 0.0), axis=1, keepdims=True)
        o_ref[...] = jnp.where(iota((per_peer, width), 1) == 0, gate, is_first)
        for fetch in fetches:
            fetch.wait()

    return pl.pallas_call(
        kernel,
        in_specs=[SMEM, VMEM] + [HBM] * count_fetched,
        out_specs=[VMEM] * (2 + count_fetched),
        out_shape=[
            jax.ShapeDtypeStruct((n_ctx * per_peer, rows_all), BF16),
            jax.ShapeDtypeStruct((per_peer, width), F32),
        ]
        + [jax.ShapeDtypeStruct((x.shape[0], columns), x.dtype) for x, columns in fetched],
        scratch_shapes=[pltpu.SemaphoreType.DMA((count_fetched,))],
        compiler_params=pltpu.CompilerParams(vmem_limit_bytes=LIMIT),
        name="selection",
    )(place, parts, *[in_hbm(x) for x, columns in fetched])


def dispatch(partials, picks, n_ctx, n_head, n_pair):
    _, _, columns = partials.shape
    per_peer = picks.shape[0] // n_ctx

    def kernel(x_ref, d_ref, o_ref):
        halves = []
        for p in range(n_pair):
            acc = x_ref[p].astype(F32)
            for h in range(1, n_head):
                acc = acc + x_ref[h * n_pair + p].astype(F32)
            halves.append(acc)
        hidden = jnp.concatenate(halves, axis=0).astype(BF16)
        o_ref[...] = dot(d_ref[...], hidden).reshape(n_ctx, per_peer, columns).astype(BF16)

    return pl.pallas_call(
        kernel,
        out_shape=jax.ShapeDtypeStruct((n_ctx, per_peer, columns), BF16),
        compiler_params=pltpu.CompilerParams(vmem_limit_bytes=LIMIT),
        name="dispatch",
    )(partials, picks)


def chunk_of(units):
    return 256 if units % 256 == 0 else units


def run_expert(parts, slot_facts, gain, early, gate_up, down):
    sources, slots, columns = parts.shape
    capacity = slots // sources
    width = sources * columns
    units = down.shape[0]
    chunk = chunk_of(units)
    count = units // chunk
    starts = [units]
    for i in range(1, count):
        starts += [i * chunk, units + i * chunk]

    def kernel(x_ref, f_ref, g_ref, early_ref, up_hbm, down_hbm, y_ref, up_ref, down_ref, sems):
        ups = [
            pltpu.make_async_copy(up_hbm.at[:, pl.ds(start, chunk)], up_ref.at[i], sems.at[i])
            for i, start in enumerate(starts)
        ]
        downs = [
            pltpu.make_async_copy(
                down_hbm.at[pl.ds(i * chunk, chunk)], down_ref.at[pl.ds(i * chunk, chunk)], sems.at[len(starts) + i]
            )
            for i in range(count)
        ]
        for copy in ups + downs:
            copy.start()
        rows = jnp.concatenate([x_ref[s].astype(F32) for s in range(sources)], axis=1)
        mean = jnp.sum(rows * rows, axis=1, keepdims=True) * (1.0 / width)
        normed = (rows * lax.rsqrt(mean + 1e-06) * g_ref[...]).astype(BF16)
        inner = []
        for i in range(count):
            if i == 0:
                gate = dot(normed, early_ref[...])
            else:
                ups[2 * i - 1].wait()
                gate = dot(normed, up_ref[2 * i - 1])
            ups[2 * i].wait()
            inner.append((gate / (1.0 + jnp.exp(-gate)) * dot(normed, up_ref[2 * i])).astype(BF16))
        out = jnp.zeros((slots, width), F32)
        for i in range(count):
            downs[i].wait()
            out = out + dot(inner[i], down_ref[i * chunk : (i + 1) * chunk, :])
        out = out * f_ref[:, 0:1] + rows * f_ref[:, 1:2]
        y_ref[...] = out.astype(BF16).reshape(sources, capacity, width)

    return pl.pallas_call(
        kernel,
        in_specs=[VMEM, VMEM, VMEM, VMEM, HBM, HBM],
        out_shape=jax.ShapeDtypeStruct((sources, capacity, width), BF16),
        scratch_shapes=[
            pltpu.VMEM((len(starts), width, chunk), BF16),
            pltpu.VMEM(down.shape, BF16),
            pltpu.SemaphoreType.DMA((len(starts) + count,)),
        ],
        compiler_params=pltpu.CompilerParams(vmem_limit_bytes=24 << 20),
        name="run_expert",
    )(parts, slot_facts, gain.reshape(1, width), early, in_hbm(gate_up), in_hbm(down))


def sum_rows(returned, lists, place, sizes):
    n_ctx, n_head, n_pair, rows_own, top, capacity = sizes
    slots, width = n_ctx * capacity, returned.shape[2]
    rows = lists.shape[1]

    def kernel(place_ref, x_ref, l_ref, o_ref):
        slot = iota((slots, rows), 0)
        expert = slot // capacity * n_head * n_pair + place_ref[0] * n_pair + place_ref[1]
        hits = jnp.zeros((slots, rows), F32)
        for k in range(top):
            hits = jnp.where(l_ref[k : k + 1, :] == expert, 1.0, hits)
        earlier = (iota((rows, rows), 0) < iota((rows, rows), 1)).astype(F32).astype(BF16)
        rank = dot(hits.astype(BF16), earlier)
        taken = jnp.where(rank == (slot % capacity).astype(F32), hits, 0.0).astype(BF16)
        x = x_ref[...].reshape(slots, width)
        out = lax.dot_general(taken, x, (((0,), (0,)), ((), ())), preferred_element_type=F32)
        o_ref[...] = out.reshape(n_head * n_pair, rows_own, width)

    return pl.pallas_call(
        kernel,
        in_specs=[SMEM, VMEM, VMEM],
        out_shape=jax.ShapeDtypeStruct((n_head * n_pair, rows_own, width), F32),
        compiler_params=pltpu.CompilerParams(vmem_limit_bytes=LIMIT),
        name="sum_rows",
    )(place, returned, lists)


def finish(shares):
    def kernel(x_ref, o_ref):
        o_ref[...] = jnp.sum(x_ref[...], axis=0).astype(BF16)

    return pl.pallas_call(
        kernel,
        out_shape=jax.ShapeDtypeStruct(shares.shape[1:], BF16),
        compiler_params=pltpu.CompilerParams(vmem_limit_bytes=LIMIT),
        name="finish",
    )(shares)


def body(
    queries,
    prompt_keys,
    prompt_values,
    residual,
    out_weight,
    norm_gain,
    expert_lists,
    gate_weights,
    gate_up,
    down_proj,
):
    n_ctx = lax.axis_size("ctx")
    n_head = lax.axis_size("head")
    n_pair = lax.axis_size("pair")
    rows_own, _ = residual.shape
    _, heads, head_size = queries.shape
    _, top = expert_lists.shape
    capacity = 2
    rows_half = n_head * rows_own
    pairs_block = rows_half * heads
    sizes = (n_ctx, n_head, n_pair, rows_own, top, capacity)
    head, pair = lax.axis_index("head"), lax.axis_index("pair")
    ctx = lax.axis_index("ctx")
    place = jnp.stack([head, pair, ctx, ctx % 2]).astype(jnp.int32)

    quarters = queries.reshape(n_ctx // 2, 2, n_head, n_pair, rows_own * heads, head_size)
    keys = prompt_keys.reshape(-1, head_size)
    values = prompt_values.reshape(-1, head_size)
    lists, weights = expert_lists.T, gate_weights.T
    cores = [(i, i ^ 1) for i in range(n_pair)]
    chips = [(i, i ^ 1) for i in range(n_ctx)]
    parities = [list(range(i, n_ctx, 2)) for i in range(2)]
    away, q_two, q_three, q_four, keys, values, residual, facts = attend_first(
        place, quarters, keys, values, residual, lists, weights, pairs_block
    )
    swapped = lax.ppermute(away, "pair", cores)
    here = attend_next(q_two, keys, values, pairs_block)
    passed = merge((here, swapped), residual, facts, place, True)
    passed, q_three, q_four = lax.optimization_barrier((passed, q_three, q_four))
    from_chip = lax.ppermute(passed, "ctx", chips)
    away = attend_next(q_three, keys, values, pairs_block)
    away, q_four = lax.optimization_barrier((away, q_four))
    swapped = lax.ppermute(away, "pair", cores)
    here = attend_next(q_four, keys, values, pairs_block)
    merged = merge((here, swapped, from_chip), residual, facts, place, False)
    parts = lax.all_to_all(merged, "ctx", 0, 0, axis_index_groups=parities, tiled=True)
    copies = combine_all(parts, rows_half, heads, n_ctx)
    gate_up_here = gate_up[0]
    early = chunk_of(down_proj.shape[1])
    picks, slot_facts, weight_here, early_here = selection(
        parts, place, sizes, ((out_weight, out_weight.shape[1]), (gate_up_here, early))
    )
    attended = lax.all_to_all(copies, "ctx", 0, 0, tiled=True)
    attended, picks, slot_facts = lax.optimization_barrier((attended, picks, slot_facts))
    partial = project(attended, weight_here, parts, place, rows_half, heads, n_head * n_pair)
    partials = lax.all_to_all(partial, ("head", "pair"), 0, 0, tiled=True)
    sending = dispatch(partials, picks, n_ctx, n_head, n_pair)
    arrived = lax.all_to_all(sending, "ctx", 0, 0, tiled=True)
    produced = run_expert(arrived, slot_facts, norm_gain, early_here, gate_up_here, down_proj[0])
    returned = lax.all_to_all(produced, "ctx", 0, 0, tiled=True)
    weighted = sum_rows(returned, lists, place, sizes)
    shares = lax.all_to_all(weighted, ("head", "pair"), 0, 0, tiled=True)
    return finish(shares)


def solution(mesh):
    in_specs = (
        P("groups", "head", None),
        P(("groups", "ctx", "pair"), "head", None),
        P(("groups", "ctx", "pair"), "head", None),
        P(("groups", "ctx", "head", "pair"), None),
        P("head", "ctx"),
        P(),
        P(("groups", "ctx"), None),
        P(("groups", "ctx"), None),
        P(("ctx", "head", "pair"), None, None),
        P(("ctx", "head", "pair"), None, None),
    )
    out_specs = P(("groups", "ctx", "head", "pair"), None)
    return jax.shard_map(body, mesh=mesh, in_specs=in_specs, out_specs=out_specs, check_vma=False)
```

```python
import functools
import math

import jax
import jax.numpy as jnp
from jax import lax
from jax.experimental import pallas as pl
from jax.experimental.pallas import tpu as pltpu
from jax.sharding import PartitionSpec as P


F32 = jnp.float32
BF16 = jnp.bfloat16
LIMIT = 16 << 20
LOG2E = math.log2(math.e)
STATS = 8


SMEM = pl.BlockSpec(memory_space=pltpu.SMEM)
VMEM = pl.BlockSpec(memory_space=pltpu.VMEM)
HBM = pl.BlockSpec(memory_space=pltpu.HBM)


def in_hbm(x):
    return pltpu.with_memory_space_constraint(x, pltpu.HBM)


def iota(shape, dim):
    return lax.broadcasted_iota(jnp.int32, shape, dim)


def dot(a, b):
    return lax.dot_general(a, b, (((1,), (0,)), ((), ())), preferred_element_type=F32)


def as_row(column, lanes):
    n = column.shape[0]
    here = iota((n, lanes), 0) == iota((n, lanes), 1)
    return jnp.sum(jnp.where(here, jnp.broadcast_to(column, (n, lanes)), 0.0), axis=0, keepdims=True)


def as_column(row, n):
    lanes = row.shape[1]
    here = iota((n, lanes), 0) == iota((n, lanes), 1)
    return jnp.sum(jnp.where(here, jnp.broadcast_to(row, (n, lanes)), 0.0), axis=1, keepdims=True)


def pieces(row):
    first = row.astype(BF16).astype(F32)
    second = (row - first).astype(BF16).astype(F32)
    third = row - first - second
    return first, second, third


def stacked(rows, lanes):
    at = iota((STATS, lanes), 0)
    out = jnp.zeros((STATS, lanes), F32)
    for i, row in enumerate(rows):
        out = jnp.where(at == i, jnp.broadcast_to(row, (STATS, lanes)), out)
    return out


def attend_tiles(q_ref, k_ref, v_ref, o_ref, score_refs, pairs_block, ready):
    blocks, _, _, width = q_ref.shape
    tile_blocks = max(1, 128 // pairs_block)
    tile = tile_blocks * pairs_block
    steps = blocks // tile_blocks
    scale = LOG2E / math.sqrt(width)

    def scores(i):
        q = q_ref[i * tile_blocks : (i + 1) * tile_blocks].reshape(tile, width)
        score_refs[i % 2][...] = lax.dot_general(
            q, k_ref[...], (((1,), (1,)), ((), ())), preferred_element_type=F32
        )

    scores(0)
    ready()
    for i in range(steps):
        if i + 1 < steps:
            scores(i + 1)
        here = score_refs[i % 2][...]
        top = jnp.max(here, axis=1, keepdims=True)
        probs = jnp.exp2((here - top) * scale)
        total = jnp.sum(probs, axis=1, keepdims=True)
        out = dot(probs.astype(BF16), v_ref[...]) / total
        level = top * scale + jnp.log(total) * LOG2E
        for b in range(tile_blocks):
            part = slice(b * pairs_block, (b + 1) * pairs_block)
            at = i * tile_blocks + b
            o_ref[at, 0:pairs_block, :] = out[part].astype(BF16)
            row = as_row(level[part], width)
            o_ref[at, pairs_block : pairs_block + STATS, :] = stacked(pieces(row), width).astype(BF16)


def attend_first(place, queries, keys, values, residual, names, weights, pairs_block):
    blocks, _, n_head, _, unit, width = queries.shape
    length = keys.shape[0]
    quarter = (blocks, n_head, unit, width)
    tile = max(1, 128 // pairs_block) * pairs_block

    def kernel(
        place_ref, q_hbm, k_hbm, v_hbm, r_hbm, n_hbm, g_hbm,
        o_ref, q2, q3, q4, k_ref, v_ref, r_ref, facts_ref,
        q1, score_a, score_b, n_ref, g_ref, sems,
    ):
        pair, parity = place_ref[1], place_ref[3]
        small = [
            pltpu.make_async_copy(a, b, sems.at[6 + i])
            for i, (a, b) in enumerate(((r_hbm, r_ref), (n_hbm, n_ref), (g_hbm, g_ref)))
        ]
        copy_k = pltpu.make_async_copy(k_hbm, k_ref, sems.at[0])
        copy_v = pltpu.make_async_copy(v_hbm, v_ref, sems.at[1])
        choices = ((q1, 1 - parity, 1 - pair), (q2, 1 - parity, pair), (q3, parity, 1 - pair), (q4, parity, pair))
        copies = [
            pltpu.make_async_copy(q_hbm.at[:, side, :, core], ref, sems.at[2 + i])
            for i, (ref, side, core) in enumerate(choices)
        ]
        copies[0].start()
        copy_k.start()
        copy_v.start()
        for copy in small:
            copy.start()
        for copy in copies[1:]:
            copy.start()

        def ready():
            copy_v.wait()
            for copy in small:
                copy.wait()
            top, rows = n_ref.shape
            spread = (iota((rows, width), 1) % rows == iota((rows, width), 0)).astype(F32).astype(BF16)
            kept = iota((top, width), 1) // rows == iota((top, width), 0)

            def in_lanes(table):
                return jnp.sum(jnp.where(kept, dot(table.astype(BF16), spread), 0.0), axis=0, keepdims=True)

            gates = g_ref[...]
            rounded = gates.astype(BF16).astype(F32)
            facts = (in_lanes(n_ref[...].astype(F32)), in_lanes(rounded), in_lanes(gates - rounded))
            facts_ref[...] = stacked(facts, width)

        copies[0].wait()
        copy_k.wait()
        attend_tiles(q1, k_ref, v_ref, o_ref, (score_a, score_b), pairs_block, ready)
        for copy in copies[1:]:
            copy.wait()

    return pl.pallas_call(
        kernel,
        in_specs=[SMEM] + [HBM] * 6,
        out_specs=[VMEM] * 8,
        out_shape=[jax.ShapeDtypeStruct((blocks, pairs_block + STATS, width), BF16)]
        + [jax.ShapeDtypeStruct(quarter, BF16)] * 3
        + [jax.ShapeDtypeStruct(x.shape, BF16) for x in (keys, values, residual)]
        + [jax.ShapeDtypeStruct((STATS, width), F32)],
        scratch_shapes=[pltpu.VMEM(quarter, BF16)]
        + [pltpu.VMEM((tile, length), F32)] * 2
        + [pltpu.VMEM(names.shape, names.dtype), pltpu.VMEM(weights.shape, weights.dtype)]
        + [pltpu.SemaphoreType.DMA((9,))],
        compiler_params=pltpu.CompilerParams(vmem_limit_bytes=LIMIT),
        name="attend_first",
    )(place, *[in_hbm(x) for x in (queries, keys, values, residual, names, weights)])


def attend_next(queries, keys, values, pairs_block):
    blocks, _, _, width = queries.shape
    tile = max(1, 128 // pairs_block) * pairs_block

    def kernel(q_ref, k_ref, v_ref, o_ref, score_a, score_b):
        attend_tiles(q_ref, k_ref, v_ref, o_ref, (score_a, score_b), pairs_block, lambda: None)

    return pl.pallas_call(
        kernel,
        in_specs=[VMEM] * 3,
        out_shape=jax.ShapeDtypeStruct((blocks, pairs_block + STATS, width), BF16),
        scratch_shapes=[pltpu.VMEM((tile, keys.shape[0]), F32)] * 2,
        compiler_params=pltpu.CompilerParams(vmem_limit_bytes=LIMIT),
        name="attend_next",
    )(queries, keys, values)


def levels_of(ref, pairs_block):
    stats = ref[:, pairs_block : pairs_block + STATS, :].astype(F32)
    return stats[:, 0, :] + stats[:, 1, :] + stats[:, 2, :]


def merge(partials, residual, facts, place, theirs):
    count = len(partials)
    blocks, height, width = partials[0].shape
    pairs_block = height - STATS
    height_out = height + STATS * (count - 2)

    def kernel(place_ref, *refs):
        parts, (r_ref, f_ref, o_ref) = refs[:count], refs[count:]
        levels = [levels_of(ref, pairs_block) for ref in parts]
        highest = functools.reduce(jnp.maximum, levels)
        shares = [jnp.exp2(level - highest) for level in levels]
        total = functools.reduce(jnp.add, shares)
        shares = [share / total for share in shares]
        first, second, third = pieces(highest + jnp.log(total) * LOG2E)
        for b in range(blocks):
            merged = jnp.zeros((pairs_block, width), F32)
            for ref, share in zip(parts, shares):
                merged = merged + ref[b, 0:pairs_block, :].astype(F32) * as_column(share[b : b + 1], pairs_block)
            o_ref[b, 0:pairs_block, :] = merged.astype(BF16)
        residual_all = r_ref[...].astype(F32)
        facts = tuple(f_ref[i : i + 1, :] for i in range(3))
        side = 1 - place_ref[3] if theirs else place_ref[3]
        for b in range(blocks):
            even = residual_all[:, 2 * b * width : (2 * b + 1) * width]
            odd = residual_all[:, (2 * b + 1) * width : (2 * b + 2) * width]
            own = jnp.where(jnp.broadcast_to(side, even.shape) == 0, even, odd)
            rows_b = (first[b : b + 1], second[b : b + 1], third[b : b + 1], own[0:1], own[1:2])
            o_ref[b, pairs_block:height, :] = stacked(rows_b + facts, width).astype(BF16)
            for ref in parts[2:]:
                o_ref[b, height:height_out, :] = ref[b, pairs_block:height, :]

    return pl.pallas_call(
        kernel,
        in_specs=[SMEM] + [VMEM] * (count + 2),
        out_shape=jax.ShapeDtypeStruct((blocks, height_out, width), BF16),
        compiler_params=pltpu.CompilerParams(vmem_limit_bytes=LIMIT),
        name="merge",
    )(place, *partials, residual, facts)


def combine_all(parts, rows_half, heads, peers):
    sources, height, width = parts.shape
    pairs_block = height - 2 * STATS

    def kernel(x_ref, o_hbm, acc_ref, att_ref, sem):
        level = levels_of(x_ref, pairs_block)
        share = jnp.exp2(level - jnp.max(level, axis=0, keepdims=True))
        share = share / jnp.sum(share, axis=0, keepdims=True)
        acc = jnp.zeros((pairs_block, width), F32)
        for s in range(sources):
            acc = acc + x_ref[s, 0:pairs_block, :].astype(F32) * as_column(share[s : s + 1], pairs_block)
        acc_ref[...] = acc
        by_head = [acc_ref[pl.ds(h, rows_half, stride=heads), :] for h in range(heads)]
        att_ref[...] = jnp.concatenate(by_head, axis=0).astype(BF16)
        copies = [pltpu.make_async_copy(att_ref, o_hbm.at[s], sem.at[s]) for s in range(peers)]
        for copy in copies:
            copy.start()
        for copy in copies:
            copy.wait()

    return pl.pallas_call(
        kernel,
        in_specs=[VMEM],
        out_specs=HBM,
        out_shape=pltpu.HBM((peers, pairs_block, width), BF16),
        scratch_shapes=[
            pltpu.VMEM((pairs_block, width), F32),
            pltpu.VMEM((pairs_block, width), BF16),
            pltpu.SemaphoreType.DMA((peers,)),
        ],
        compiler_params=pltpu.CompilerParams(vmem_limit_bytes=LIMIT),
        name="combine_all",
    )(parts)


def project(attended, weight, parts, place, rows_half, heads, copies):
    blocks, pairs_block, width = attended.shape
    columns = weight.shape[1]
    rows = blocks * rows_half

    def kernel(place_ref, a_ref, w_ref, s_ref, o_ref):
        a = a_ref[...].astype(F32)
        by_head = [a[:, h * rows_half : (h + 1) * rows_half, :].reshape(rows, width) for h in range(heads)]
        out = dot(jnp.concatenate(by_head, axis=1).astype(BF16), w_ref[...])
        stats_all = s_ref[:, pairs_block : pairs_block + 2 * STATS, :].astype(F32)
        same, other = stats_all[:, :STATS], stats_all[:, STATS:]
        at = iota((rows_half, columns), 0)
        first = 2 * place_ref[0]
        crossed = jnp.broadcast_to(place_ref[3], (STATS, columns)).astype(F32)
        finished = []
        for block in range(blocks):
            one, two = same[block // 2], other[block // 2]
            share = 1.0 - crossed if block % 2 == 0 else crossed
            stats = one * share + two * (1.0 - share)
            added = jnp.where(at == first, stats[3:4], 0.0) + jnp.where(at == first + 1, stats[4:5], 0.0)
            finished.append(out[block * rows_half : (block + 1) * rows_half] + added)
        out = jnp.concatenate(finished, axis=0).astype(BF16)
        for i in range(copies):
            o_ref[i] = out

    return pl.pallas_call(
        kernel,
        in_specs=[SMEM, VMEM, VMEM, VMEM],
        out_shape=jax.ShapeDtypeStruct((copies, rows, columns), BF16),
        compiler_params=pltpu.CompilerParams(vmem_limit_bytes=LIMIT),
        name="project",
    )(place, attended, weight, parts)


def selection(parts, place, sizes, fetched):
    n_ctx, n_head, n_pair, rows_own, _, capacity = sizes
    block_rows = n_head * n_pair * rows_own
    rows_all = n_ctx * block_rows
    blocks, height, width = parts.shape
    per_peer = n_ctx * capacity

    def natural(lane):
        pair = lane // (rows_all // n_pair)
        rest = lane % (rows_all // n_pair)
        block = rest // (n_head * rows_own)
        head = (rest // rows_own) % n_head
        return block, (head * n_pair + pair) * rows_own + rest % rows_own

    count_fetched = len(fetched)
    starts = [start for _, start, _ in fetched]

    def kernel(place_ref, s_ref, *refs):
        sources, d_ref, o_ref = refs[:count_fetched], refs[count_fetched], refs[count_fetched + 1]
        targets, sems = refs[count_fetched + 2 : -1], refs[-1]
        fetches = [
            pltpu.make_async_copy(a.at[:, pl.ds(starts[i], b.shape[1])], b, sems.at[i])
            for i, (a, b) in enumerate(zip(sources, targets))
        ]
        for fetch in fetches:
            fetch.start()
        stats = s_ref[:, height - 2 * STATS : height, :].astype(F32)
        came = iota((n_ctx, n_ctx), 1)
        came = came % blocks * 2 + jnp.where(came < blocks, place_ref[3], 1 - place_ref[3])
        order = (came == iota((n_ctx, n_ctx), 0)).astype(F32).astype(BF16)

        def in_order(row):
            rows = jnp.concatenate([stats[:, row, :], stats[:, row + STATS, :]], axis=0)
            return dot(order, rows.astype(BF16))

        listed = in_order(5)
        count = n_ctx * n_ctx
        repeated = jnp.concatenate([listed] * n_ctx, axis=0)
        expert = (iota((count, width), 0) // n_ctx * n_head * n_pair + place_ref[0] * n_pair + place_ref[1]).astype(F32)
        equal = (repeated == expert).astype(F32).astype(BF16)
        fold = (iota((width, block_rows), 0) % block_rows == iota((width, block_rows), 1)).astype(F32).astype(BF16)
        hits = dot(equal, fold)
        earlier = (iota((block_rows, block_rows), 0) < iota((block_rows, block_rows), 1)).astype(F32).astype(BF16)
        rank = dot(hits.astype(BF16), earlier)
        slot = jnp.where(hits > 0.5, rank + 1.0, 0.0).astype(BF16)
        expand = iota((count * capacity, count), 0) // capacity == iota((count * capacity, count), 1)
        slot = dot(expand.astype(F32).astype(BF16), slot).astype(BF16)
        block, row = natural(iota((block_rows, rows_all), 1))
        spread = (iota((block_rows, rows_all), 0) == row).astype(F32).astype(BF16)
        slot = dot(slot, spread)
        at = iota((count * capacity, rows_all), 0)
        block, row = natural(iota((count * capacity, rows_all), 1))
        mine = (block == (at // capacity) % n_ctx) & (slot == (at % capacity + 1).astype(F32))
        d_ref[...] = mine.astype(F32).astype(BF16)
        own = (place_ref[2] * n_head * n_pair + place_ref[0] * n_pair + place_ref[1]).astype(F32)
        same = (listed == own).astype(F32).astype(BF16)
        rank = dot(dot(same, fold).astype(BF16), earlier).astype(BF16)
        back = (iota((block_rows, width), 1) % block_rows == iota((block_rows, width), 0)).astype(F32).astype(BF16)
        twice = iota((per_peer, n_ctx), 0) // capacity == iota((per_peer, n_ctx), 1)
        twice = twice.astype(F32).astype(BF16)
        rank = dot(twice, dot(rank, back).astype(BF16))
        used = (dot(twice, same) > 0.5) & (rank == (iota((per_peer, width), 0) % capacity).astype(F32))
        gates = dot(twice, in_order(6).astype(BF16)) + dot(twice, in_order(7).astype(BF16))
        gate = jnp.sum(jnp.where(used, gates, 0.0), axis=1, keepdims=True)
        is_first = used & (iota((per_peer, width), 1) < block_rows)
        is_first = jnp.sum(jnp.where(is_first, 1.0, 0.0), axis=1, keepdims=True)
        o_ref[...] = jnp.where(iota((per_peer, width), 1) == 0, gate, is_first)
        for fetch in fetches:
            fetch.wait()

    return pl.pallas_call(
        kernel,
        in_specs=[SMEM, VMEM] + [HBM] * count_fetched,
        out_specs=[VMEM] * (2 + count_fetched),
        out_shape=[
            jax.ShapeDtypeStruct((n_ctx * per_peer, rows_all), BF16),
            jax.ShapeDtypeStruct((per_peer, width), F32),
        ]
        + [jax.ShapeDtypeStruct((x.shape[0], columns), x.dtype) for x, _, columns in fetched],
        scratch_shapes=[pltpu.SemaphoreType.DMA((count_fetched,))],
        compiler_params=pltpu.CompilerParams(vmem_limit_bytes=LIMIT),
        name="selection",
    )(place, parts, *[in_hbm(x) for x, _, columns in fetched])


def dispatch(partials, picks, n_ctx, n_head, n_pair):
    _, _, columns = partials.shape
    per_peer = picks.shape[0] // n_ctx

    def kernel(x_ref, d_ref, o_ref):
        halves = []
        for p in range(n_pair):
            acc = x_ref[p].astype(F32)
            for h in range(1, n_head):
                acc = acc + x_ref[h * n_pair + p].astype(F32)
            halves.append(acc)
        hidden = jnp.concatenate(halves, axis=0).astype(BF16)
        o_ref[...] = dot(d_ref[...], hidden).reshape(n_ctx, per_peer, columns).astype(BF16)

    return pl.pallas_call(
        kernel,
        out_shape=jax.ShapeDtypeStruct((n_ctx, per_peer, columns), BF16),
        compiler_params=pltpu.CompilerParams(vmem_limit_bytes=LIMIT),
        name="dispatch",
    )(partials, picks)


def chunk_of(units):
    return 256 if units % 256 == 0 else units


def run_expert(parts, slot_facts, gain, early_gate, early_up, gate_up, down):
    sources, slots, columns = parts.shape
    capacity = slots // sources
    width = sources * columns
    units = down.shape[0]
    chunk = chunk_of(units)
    count = units // chunk
    starts = []
    for i in range(1, count):
        starts += [i * chunk, units + i * chunk]

    def kernel(x_ref, f_ref, g_ref, eg_ref, eu_ref, up_hbm, down_hbm, y_ref, up_ref, down_ref, sems):
        ups = [
            pltpu.make_async_copy(up_hbm.at[:, pl.ds(start, chunk)], up_ref.at[i], sems.at[i])
            for i, start in enumerate(starts)
        ]
        downs = [
            pltpu.make_async_copy(
                down_hbm.at[pl.ds(i * chunk, chunk)], down_ref.at[pl.ds(i * chunk, chunk)], sems.at[len(starts) + i]
            )
            for i in range(count)
        ]
        for copy in ups + downs:
            copy.start()
        rows = jnp.concatenate([x_ref[s].astype(F32) for s in range(sources)], axis=1)
        mean = jnp.sum(rows * rows, axis=1, keepdims=True) * (1.0 / width)
        normed = (rows * lax.rsqrt(mean + 1e-06) * g_ref[...]).astype(BF16)
        inner = []
        for i in range(count):
            if i == 0:
                gate, up = dot(normed, eg_ref[...]), dot(normed, eu_ref[...])
            else:
                ups[2 * i - 2].wait()
                gate = dot(normed, up_ref[2 * i - 2])
                ups[2 * i - 1].wait()
                up = dot(normed, up_ref[2 * i - 1])
            inner.append((gate / (1.0 + jnp.exp(-gate)) * up).astype(BF16))
        out = jnp.zeros((slots, width), F32)
        for i in range(count):
            downs[i].wait()
            out = out + dot(inner[i], down_ref[i * chunk : (i + 1) * chunk, :])
        out = out * f_ref[:, 0:1] + rows * f_ref[:, 1:2]
        y_ref[...] = out.astype(BF16).reshape(sources, capacity, width)

    return pl.pallas_call(
        kernel,
        in_specs=[VMEM] * 5 + [HBM] * 2,
        out_shape=jax.ShapeDtypeStruct((sources, capacity, width), BF16),
        scratch_shapes=[
            pltpu.VMEM((len(starts), width, chunk), BF16),
            pltpu.VMEM(down.shape, BF16),
            pltpu.SemaphoreType.DMA((len(starts) + count,)),
        ],
        compiler_params=pltpu.CompilerParams(vmem_limit_bytes=24 << 20),
        name="run_expert",
    )(parts, slot_facts, gain.reshape(1, width), early_gate, early_up, in_hbm(gate_up), in_hbm(down))


def sum_rows(returned, lists, place, sizes):
    n_ctx, n_head, n_pair, rows_own, top, capacity = sizes
    slots, width = n_ctx * capacity, returned.shape[2]
    rows = lists.shape[1]

    def kernel(place_ref, x_ref, l_ref, o_ref):
        slot = iota((slots, rows), 0)
        expert = slot // capacity * n_head * n_pair + place_ref[0] * n_pair + place_ref[1]
        hits = jnp.zeros((slots, rows), F32)
        for k in range(top):
            hits = jnp.where(l_ref[k : k + 1, :] == expert, 1.0, hits)
        earlier = (iota((rows, rows), 0) < iota((rows, rows), 1)).astype(F32).astype(BF16)
        rank = dot(hits.astype(BF16), earlier)
        taken = jnp.where(rank == (slot % capacity).astype(F32), hits, 0.0).astype(BF16)
        x = x_ref[...].reshape(slots, width)
        out = lax.dot_general(taken, x, (((0,), (0,)), ((), ())), preferred_element_type=F32)
        o_ref[...] = out.astype(BF16).reshape(n_head * n_pair, rows_own, width)

    return pl.pallas_call(
        kernel,
        in_specs=[SMEM, VMEM, VMEM],
        out_shape=jax.ShapeDtypeStruct((n_head * n_pair, rows_own, width), BF16),
        compiler_params=pltpu.CompilerParams(vmem_limit_bytes=LIMIT),
        name="sum_rows",
    )(place, returned, lists)


def finish(shares):
    def kernel(x_ref, o_ref):
        o_ref[...] = jnp.sum(x_ref[...].astype(F32), axis=0).astype(BF16)

    return pl.pallas_call(
        kernel,
        out_shape=jax.ShapeDtypeStruct(shares.shape[1:], BF16),
        compiler_params=pltpu.CompilerParams(vmem_limit_bytes=LIMIT),
        name="finish",
    )(shares)


def body(
    queries,
    prompt_keys,
    prompt_values,
    residual,
    out_weight,
    norm_gain,
    expert_lists,
    gate_weights,
    gate_up,
    down_proj,
):
    n_ctx = lax.axis_size("ctx")
    n_head = lax.axis_size("head")
    n_pair = lax.axis_size("pair")
    rows_own, _ = residual.shape
    _, heads, head_size = queries.shape
    _, top = expert_lists.shape
    capacity = 2
    rows_half = n_head * rows_own
    pairs_block = rows_half * heads
    sizes = (n_ctx, n_head, n_pair, rows_own, top, capacity)
    head, pair = lax.axis_index("head"), lax.axis_index("pair")
    ctx = lax.axis_index("ctx")
    place = jnp.stack([head, pair, ctx, ctx % 2]).astype(jnp.int32)

    quarters = queries.reshape(n_ctx // 2, 2, n_head, n_pair, rows_own * heads, head_size)
    keys = prompt_keys.reshape(-1, head_size)
    values = prompt_values.reshape(-1, head_size)
    lists, weights = expert_lists.T, gate_weights.T
    cores = [(i, i ^ 1) for i in range(n_pair)]
    chips = [(i, i ^ 1) for i in range(n_ctx)]
    parities = [list(range(i, n_ctx, 2)) for i in range(2)]
    away, q_two, q_three, q_four, keys, values, residual, facts = attend_first(
        place, quarters, keys, values, residual, lists, weights, pairs_block
    )
    swapped = lax.ppermute(away, "pair", cores)
    here = attend_next(q_two, keys, values, pairs_block)
    passed = merge((here, swapped), residual, facts, place, True)
    passed, q_three, q_four = lax.optimization_barrier((passed, q_three, q_four))
    from_chip = lax.ppermute(passed, "ctx", chips)
    away = attend_next(q_three, keys, values, pairs_block)
    away, q_four = lax.optimization_barrier((away, q_four))
    swapped = lax.ppermute(away, "pair", cores)
    here = attend_next(q_four, keys, values, pairs_block)
    merged = merge((here, swapped, from_chip), residual, facts, place, False)
    parts = lax.all_to_all(merged, "ctx", 0, 0, axis_index_groups=parities, tiled=True)
    copies = combine_all(parts, rows_half, heads, n_ctx)
    gate_up_here = gate_up[0]
    early = chunk_of(down_proj.shape[1])
    picks, slot_facts, weight_here, early_gate, early_up = selection(
        parts, place, sizes, ((out_weight, 0, out_weight.shape[1]), (gate_up_here, 0, early), (gate_up_here, down_proj.shape[1], early))
    )
    attended = lax.all_to_all(copies, "ctx", 0, 0, tiled=True)
    attended, picks, slot_facts = lax.optimization_barrier((attended, picks, slot_facts))
    partial = project(attended, weight_here, parts, place, rows_half, heads, n_head * n_pair)
    partials = lax.all_to_all(partial, ("head", "pair"), 0, 0, tiled=True)
    sending = dispatch(partials, picks, n_ctx, n_head, n_pair)
    arrived = lax.all_to_all(sending, "ctx", 0, 0, tiled=True)
    produced = run_expert(arrived, slot_facts, norm_gain, early_gate, early_up, gate_up_here, down_proj[0])
    returned = lax.all_to_all(produced, "ctx", 0, 0, tiled=True)
    weighted = sum_rows(returned, lists, place, sizes)
    shares = lax.all_to_all(weighted, ("head", "pair"), 0, 0, tiled=True)
    return finish(shares)


def solution(mesh):
    in_specs = (
        P("groups", "head", None),
        P(("groups", "ctx", "pair"), "head", None),
        P(("groups", "ctx", "pair"), "head", None),
        P(("groups", "ctx", "head", "pair"), None),
        P("head", "ctx"),
        P(),
        P(("groups", "ctx"), None),
        P(("groups", "ctx"), None),
        P(("ctx", "head", "pair"), None, None),
        P(("ctx", "head", "pair"), None, None),
    )
    out_specs = P(("groups", "ctx", "head", "pair"), None)
    return jax.shard_map(body, mesh=mesh, in_specs=in_specs, out_specs=out_specs, check_vma=False)
```
